256 devices in a mesh: zero: 8 (over z), width: 16 (over y, x), unit: 2 (over core).
Axes of the slice: x: 4, y: 4, z: 8, core: 2. Of those that a mesh axis runs over, the one named last changes fastest.
Arguments:
- train_query: bfloat16 [8192, 4096], P(('unit', 'zero'), 'width'), parts along dimension 0, may hold values from -0.125 to 0.125
- low_query: bfloat16 [8192, 16], P(('unit', 'zero')), parts along dimension 0, may hold values from -0.09375 to 0.09375
- high_query: bfloat16 [32, 4096], P('unit', 'width'), parts along dimension 0, may hold values from -1.5 to 1.5
- train_key: bfloat16 [8192, 4096], P(('unit', 'zero'), 'width'), parts along dimension 0, may hold values from -0.125 to 0.125
- low_key: bfloat16 [8192, 16], P(('unit', 'zero')), parts along dimension 0, may hold values from -0.09375 to 0.09375
- high_key: bfloat16 [32, 4096], P('unit', 'width'), parts along dimension 0, may hold values from -1.5 to 1.5
- train_value: bfloat16 [8192, 4096], P(('unit', 'zero'), 'width'), parts along dimension 0, may hold values from -0.125 to 0.125
- low_value: bfloat16 [8192, 16], P(('unit', 'zero')), parts along dimension 0, may hold values from -0.09375 to 0.09375
- high_value: bfloat16 [32, 4096], P('unit', 'width'), parts along dimension 0, may hold values from -1.5 to 1.5
- norm_train: float32 [8192], P(('unit', 'zero', 'width')), parts along dimension 0, may hold values from 0.25 to 1.75
- norm_step: float32 [8192], P(('unit', 'zero', 'width')), parts along dimension 0, may hold values from -0.3 to 0.3
Outputs:
- serve_query: bfloat16 [8192, 4096], P('unit', 'width'), parts along dimension 0
- serve_key: bfloat16 [8192, 4096], P('unit', 'width'), parts along dimension 0
- serve_value: bfloat16 [8192, 4096], P('unit', 'width'), parts along dimension 0
- factor_query: float32 [8192], P(('unit', 'width')), parts along dimension 0
- factor_key: float32 [8192], P(('unit', 'width')), parts along dimension 0
- factor_value: float32 [8192], P(('unit', 'width')), parts along dimension 0
- serve_norm: bfloat16 [8192], P('unit'), parts along dimension 0
The draws below stay inside these ranges and needn't reach their ends.
There are 2 independent parts, one for each index of `unit`. The reference program is written for one: setup_inputs(seed, part) draws one part's arguments, and reference() takes and returns one part's arrays. A program takes and returns all parts, laid end to end along the dimension named above; each array names one. Nothing has to cross between parts.
All inputs are finite; a program needn't handle non-finite values. Where the reference program divides by a largest or mean magnitude, that divisor is 1e-20 or more.
Results may differ from the reference program's by a relative error of at most 0.001.
Values may be sent and summed in bfloat16 or wider, within the bound.
A program may use at most 64 MiB of HBM per device.

```python
import jax
import jax.numpy as jnp

D_MODEL = 4096
Q_DIM = 4096
KV_DIM = 4096
RANK = 16


def with_spikes(drawn, key, source, target, parts, factor):
    owner, partner = [(jnp.arange(drawn.shape[axis_at]) // (drawn.shape[axis_at] // parts)).reshape([-1 if axis == axis_at else 1 for axis in range(drawn.ndim)]) for axis_at in (source, target)]
    chosen = jax.random.permutation(key, parts)[partner]
    strong = (owner == chosen) | (owner == (partner + parts // 2) % parts)
    return jnp.where(strong, factor * drawn, drawn)


def level_of(rng, dims, split, least, largest):
    factor_of = 1.0
    for axis_at, blocks in split:
        steps = jax.random.uniform(jax.random.fold_in(jax.random.fold_in(rng, 6), axis_at), (blocks,), jnp.float32, least / len(split), largest / len(split))
        factor_of = factor_of * jnp.repeat(jnp.exp(steps), dims[axis_at] // blocks).reshape((-1,) + (1,) * (len(dims) - 1 - axis_at))
    return factor_of


def scatter_about(key, dims, deviation, most, split=(), kind=jnp.bfloat16):
    entries = deviation * jax.random.normal(key, dims, jnp.float32)
    if split:
        entries = entries * level_of(key, dims, split, -0.22, 0.18)
    return jnp.clip(entries, -most, most).astype(kind)


def noise_with(rng, shape, scale, most, split, heavy, held_as=jnp.bfloat16):
    array = scale * jax.random.normal(rng, shape, jnp.float32)
    if split:
        array = array * level_of(rng, shape, split, -0.22, 0.18)
    return jnp.clip(with_spikes(array, jax.random.fold_in(rng, 3), *heavy), -most, most).astype(held_as)


def setup_inputs(seed: int = 0, part: int = 0) -> dict:
    seeds = jax.random.split(jax.random.key(seed), 12)
    part_splits = jax.random.split(jax.random.fold_in(seeds[11], part), 12)
    train_query = noise_with(part_splits[0], (D_MODEL, Q_DIM), D_MODEL ** -0.5, 0.125, ((0, 8), (1, 16)), (0, 1, 16, 2.0))
    low_query = scatter_about(part_splits[1], (D_MODEL, RANK), D_MODEL ** -0.5, 0.09375, ((0, 8),))
    high_query = scatter_about(part_splits[2], (RANK, Q_DIM), RANK ** -0.5, 1.5, ((1, 16),))
    train_key = noise_with(part_splits[3], (D_MODEL, KV_DIM), D_MODEL ** -0.5, 0.125, ((0, 8), (1, 16)), (0, 1, 16, 2.0))
    low_key = scatter_about(part_splits[4], (D_MODEL, RANK), D_MODEL ** -0.5, 0.09375, ((0, 8),))
    high_key = scatter_about(part_splits[5], (RANK, KV_DIM), RANK ** -0.5, 1.5, ((1, 16),))
    train_value = noise_with(part_splits[6], (D_MODEL, KV_DIM), D_MODEL ** -0.5, 0.125, ((0, 8), (1, 16)), (0, 1, 16, 2.0))
    low_value = scatter_about(part_splits[7], (D_MODEL, RANK), D_MODEL ** -0.5, 0.09375, ((0, 8),))
    high_value = scatter_about(part_splits[8], (RANK, KV_DIM), RANK ** -0.5, 1.5, ((1, 16),))
    norm_train = jnp.clip(1.0 + 0.15 * jax.random.normal(part_splits[9], (D_MODEL,), jnp.float32), 0.25, 1.75)
    norm_step = jnp.clip(jax.random.uniform(part_splits[10], (D_MODEL,), jnp.float32, -0.3, 0.3) * level_of(part_splits[10], (D_MODEL,), ((0, 128),), -0.4, 0.0), -0.3, 0.3)
    return dict(train_query=train_query, low_query=low_query, high_query=high_query, train_key=train_key, low_key=low_key, high_key=high_key, train_value=train_value, low_value=low_value, high_value=high_value, norm_train=norm_train, norm_step=norm_step)


mix_rate = 1.0


def reference(train_query, low_query, high_query, train_key, low_key, high_key, train_value, low_value, high_value, norm_train, norm_step):
    fresh_query = train_query.astype(jnp.float32) + mix_rate * jnp.dot(low_query, high_query, preferred_element_type=jnp.float32)
    fresh_key = train_key.astype(jnp.float32) + mix_rate * jnp.dot(low_key, high_key, preferred_element_type=jnp.float32)
    fresh_value = train_value.astype(jnp.float32) + mix_rate * jnp.dot(low_value, high_value, preferred_element_type=jnp.float32)
    factor_query = jnp.max(jnp.abs(fresh_query), axis=0)
    serve_query = (fresh_query / factor_query).astype(jnp.bfloat16)
    factor_key = jnp.max(jnp.abs(fresh_key), axis=0)
    serve_key = (fresh_key / factor_key).astype(jnp.bfloat16)
    factor_value = jnp.max(jnp.abs(fresh_value), axis=0)
    serve_value = (fresh_value / factor_value).astype(jnp.bfloat16)
    serve_norm = (norm_train + norm_step).astype(jnp.bfloat16)
    return serve_query, serve_key, serve_value, factor_query, factor_key, factor_value, serve_norm
```

```python
import functools

import jax
import jax.numpy as jnp
from jax import lax
from jax.experimental import pallas as pl
from jax.experimental.pallas import tpu as pltpu
from jax.sharding import Mesh
from jax.sharding import PartitionSpec as P

WIDTH = ("width_0", "width_1")
UNIT_ZERO_WIDTH = ("unit", "zero", "width_0", "width_1")
UNIT_WIDTH = ("unit", "width_0", "width_1")
MESH = pl.DeviceIdType.MESH

mix_rate = 1.0

Z = 8
ROWS = 512
COLS = 256
WHOLE = Z * ROWS
BLOCK = 128
RAW = 384
PIECE = 64
NRAW = RAW // PIECE
NBLOCK = 3 * ROWS // BLOCK
FIRST = RAW // BLOCK
META = 3 * COLS + 128


def fresh_of(low_t, high, train):
    product = lax.dot_general(
        low_t, high, (((0,), (0,)), ((), ())), preferred_element_type=jnp.float32
    )
    return train.astype(jnp.float32) + mix_rate * product


def gather_kernel(
    tq, lq, hq, tk, lk, hk, tv, lv, hv, nt, ns,
    out, factors, norm,
    train, low, high, norm_in, fresh, rawx, lowx, meta, norm_x, norm_y, inverse,
    load_sem, raw_s, raw_r, blk_s, blk_r, meta_s, meta_r, low_s, low_r, nx_s, nx_r, ny_s, ny_r,
):
    z = lax.axis_index("zero")
    y = lax.axis_index("width_0")
    x = lax.axis_index("width_1")

    loads = [
        pltpu.make_async_copy(tq, train.at[0], load_sem.at[0]),
        pltpu.make_async_copy(lq, low.at[0], load_sem.at[1]),
        pltpu.make_async_copy(hq, high.at[0], load_sem.at[2]),
        pltpu.make_async_copy(tk, train.at[1], load_sem.at[3]),
        pltpu.make_async_copy(lk, low.at[1], load_sem.at[4]),
        pltpu.make_async_copy(hk, high.at[1], load_sem.at[5]),
        pltpu.make_async_copy(tv, train.at[2], load_sem.at[6]),
        pltpu.make_async_copy(lv, low.at[2], load_sem.at[7]),
        pltpu.make_async_copy(hv, high.at[2], load_sem.at[8]),
        pltpu.make_async_copy(nt, norm_in.at[0], load_sem.at[9]),
        pltpu.make_async_copy(ns, norm_in.at[1], load_sem.at[10]),
    ]
    for load in loads:
        load.start()

    def beside(axis, at, step, size):
        return {axis: lax.rem(at + (step + size), size)}

    towards = (beside("zero", z, 1, Z), beside("zero", z, -1, Z))
    barrier = pltpu.get_barrier_semaphore()
    neighbours = towards + (
        beside("width_0", y, 1, 4), beside("width_0", y, -1, 4),
        beside("width_1", x, 1, 4), beside("width_1", x, -1, 4),
    )
    for neighbour in neighbours:
        pl.semaphore_signal(barrier, inc=1, device_id=neighbour, device_id_type=MESH)
    pl.semaphore_wait(barrier, len(neighbours))

    def origin(d, h):
        back = h - 1
        return lax.rem(z + (Z - back if d == 0 else back), Z)

    def remote(src, dst, send, recv, d):
        return pltpu.make_async_remote_copy(
            src_ref=src, dst_ref=dst, send_sem=send, recv_sem=recv,
            device_id=towards[d], device_id_type=MESH,
        )

    def half(start, size, d, h):
        return (start, size) if h < 4 else (start + d * (size // 2), size // 2)

    def raw_copy(d, h, c):
        at, size = half(c * PIECE, PIECE, d, h)
        o = origin(d, h)
        there = rawx.at[o, pl.ds(at, size)]
        here = train.at[0, pl.ds(at, size)] if h == 1 else there
        return remote(here, there, raw_s.at[d, h - 1, c], raw_r.at[d, h - 1, c], d)

    def low_copy(d, h):
        o = origin(d, h)
        there = lowx.at[o]
        here = low.at[0, :, pl.ds(0, RAW)] if h == 1 else there
        return remote(here, there, low_s.at[d, h - 1], low_r.at[d, h - 1], d)

    def meta_copy(d, h):
        o = origin(d, h)
        return remote(meta.at[o], meta.at[o], meta_s.at[d, h - 1], meta_r.at[d, h - 1], d)

    def row_of(j, o):
        return (j // 4) * WHOLE + o * ROWS + (j % 4) * BLOCK

    def block_copy(d, h, j):
        at, size = half(row_of(j, origin(d, h)), BLOCK, d, h)
        ref = out.at[pl.ds(pl.multiple_of(at, size), size)]
        return remote(ref, ref, blk_s.at[d, h - 1, j], blk_r.at[d, h - 1, j], d)

    def copies(item, h):
        if item == "meta":
            return [meta_copy(d, h) for d in ((0, 1) if h < 4 else (0,))]
        if item == "low":
            return [low_copy(d, h) for d in ((0, 1) if h < 4 else (1,))]
        return [raw_copy(d, h, item) for d in (0, 1)]

    queue = []
    sent = set()

    def left(n):
        for entry in queue[: max(0, len(queue) - n)]:
            if entry not in sent:
                sent.add(entry)
                for copy in copies(*entry):
                    copy.wait_send()

    def send(item, h, depth=3):
        left(depth - 1)
        if h > 1:
            arrived(item, h - 1)
        for copy in copies(item, h):
            copy.start()
        queue.append((item, h))

    landed = set()

    def arrived(item, h):
        if (item, h) not in landed:
            landed.add((item, h))
            for copy in copies(item, h):
                copy.wait_recv()

    loads[0].wait()
    send(0, 1)
    send(1, 1)
    for load in loads[1:]:
        load.wait()
    for m in range(3):
        top = jnp.zeros((8, COLS), jnp.float32)
        for b in range(ROWS // BLOCK):
            rows = pl.ds(b * BLOCK, BLOCK)
            block = fresh_of(low[m, :, rows], high[m], train[m, rows])
            fresh[m, rows] = block
            top = jnp.maximum(top, jnp.max(jnp.abs(block).reshape(BLOCK // 8, 8, COLS), axis=0))
        meta[z, :, pl.ds(m * COLS, COLS)] = jnp.max(top, axis=0, keepdims=True)
    gain = (norm_in[0] + norm_in[1]).astype(jnp.bfloat16)
    lane = lax.broadcasted_iota(jnp.int32, (32, 128), 1)
    entry = lax.broadcasted_iota(jnp.int32, (32, 128), 0)
    place = (lane == entry + 32 * x).astype(jnp.bfloat16)
    meta[z, :, pl.ds(3 * COLS, 128)] = jnp.dot(gain, place, preferred_element_type=jnp.float32)

    order = [
        ("meta", 1), (2, 1), (3, 1), (4, 1), ("meta", 2), (5, 1), ("low", 1), (0, 2), (1, 2),
        ("meta", 3), (2, 2), (3, 2), (4, 2), ("meta", 4), (5, 2), ("low", 2), (0, 3), (1, 3), (2, 3), (3, 3),
    ]
    for item, h in order:
        send(item, h)
    arrived("meta", 4)

    top = jnp.max(meta[:, 0, : 3 * COLS], axis=0, keepdims=True)
    for m in range(3):
        factors[pl.ds(m, 1)] = top[:, m * COLS : (m + 1) * COLS]
        inverse[m] = 1.0 / top[:, m * COLS : (m + 1) * COLS]

    def scale_own(j):
        m, r = j // 4, (j % 4) * BLOCK
        scaled = fresh[m, pl.ds(r, BLOCK)] * inverse[m]
        out[pl.ds(pl.multiple_of(row_of(j, z), BLOCK), BLOCK)] = scaled.astype(jnp.bfloat16)

    for j in range(FIRST, NBLOCK):
        scale_own(j)
        if j >= FIRST + 1:
            for d in (0, 1):
                block_copy(d, 1, j - 1).start()
    for j in range(FIRST):
        scale_own(j)
    for d in (0, 1):
        block_copy(d, 1, NBLOCK - 1).start()

    for item, h in [(4, 3), (5, 3), ("low", 3)] + [(c, 4) for c in range(NRAW)] + [("low", 4)]:
        send(item, h, depth=64)

    def pass_round(buf, at, axis, send_sem, recv_sem):
        def hop(n, slot, step):
            slot = lax.rem(at + slot + 4, 4)
            return pltpu.make_async_remote_copy(
                src_ref=buf.at[slot], dst_ref=buf.at[slot], send_sem=send_sem.at[n],
                recv_sem=recv_sem.at[n], device_id=beside(axis, at, step, 4), device_id_type=MESH,
            )
        hop(0, 0, 1).start()
        hop(1, 0, -1).start()
        hop(0, 0, 1).wait_recv()
        hop(2, -1, 1).start()
        hop(1, 0, -1).wait_recv()
        hop(2, -1, 1).wait_recv()
        for n, slot, step in ((0, 0, 1), (1, 0, -1), (2, -1, 1)):
            hop(n, slot, step).wait_send()

    norm_x[x] = meta[:, 0, 3 * COLS :]
    pass_round(norm_x, x, "width_1", nx_s, nx_r)
    norm_y[y] = jnp.sum(norm_x[...], axis=0)
    pass_round(norm_y, y, "width_0", ny_s, ny_r)
    for s in range(4):
        norm[s] = norm_y[s]

    def scale_raw(o):
        for j in range(FIRST):
            rows = pl.ds(j * BLOCK, BLOCK)
            block = fresh_of(lowx[o, :, rows], high[0], rawx[o, rows])
            at = pl.multiple_of(row_of(j, o), BLOCK)
            out[pl.ds(at, BLOCK)] = (block * inverse[0]).astype(jnp.bfloat16)

    for h in (1, 2, 3):
        for c in range(NRAW):
            arrived(c, h)
        arrived("low", h)
        scale_raw(lax.rem(z + Z - h, Z))
        scale_raw(lax.rem(z + h, Z))

    for h in (1, 2, 3):
        def forward(j, _, h=h):
            for d in (0, 1):
                block_copy(d, h, j).wait_recv()
                block_copy(d, h + 1, j).start()
            return 0
        lax.fori_loop(FIRST, NBLOCK, forward, 0)
        if h == 2:
            for c in range(NRAW):
                arrived(c, 4)
            arrived("low", 4)
            scale_raw(lax.rem(z + 4, Z))

    def finish(j, _):
        for d in (0, 1):
            block_copy(d, 4, j).wait_recv()
        return 0
    lax.fori_loop(FIRST, NBLOCK, finish, 0)

    def drain(j, _):
        for h in (1, 2, 3, 4):
            for d in (0, 1):
                block_copy(d, h, j).wait_send()
        return 0
    lax.fori_loop(FIRST, NBLOCK, drain, 0)
    left(0)


def write_kernel(weights, factors, norm, sq, sk, sv, fq, fk, fv, gain, sem):
    outs = (sq, sk, sv)
    writes = [
        pltpu.make_async_copy(weights.at[pl.ds(m * WHOLE, WHOLE)], outs[m], sem.at[m])
        for m in range(3)
    ]
    for write in writes:
        write.start()
    for m, ref in enumerate((fq, fk, fv)):
        ref[...] = factors[m]
    for z in range(Z):
        for y in range(4):
            gain[pl.ds(z * 4 + y, 1)] = norm[y, pl.ds(z, 1)].astype(jnp.bfloat16)
    for write in writes:
        write.wait()


def per_device(tq, lq, hq, tk, lk, hk, tv, lv, hv, nt, ns):
    hbm = pl.BlockSpec(memory_space=pl.ANY)
    vmem = pl.BlockSpec(memory_space=pltpu.VMEM)
    dma = pltpu.SemaphoreType.DMA
    f32, bf16 = jnp.float32, jnp.bfloat16
    weights, factors, norm = pl.pallas_call(
        gather_kernel,
        name="gather_z",
        out_shape=(
            pltpu.VMEM((3 * WHOLE, COLS), bf16),
            pltpu.VMEM((8, COLS), f32),
            pltpu.VMEM((4, Z, 128), f32),
        ),
        in_specs=[hbm] * 11,
        out_specs=(vmem, vmem, vmem),
        scratch_shapes=[
            pltpu.VMEM((3, ROWS, COLS), bf16),
            pltpu.VMEM((3, 16, ROWS), bf16),
            pltpu.VMEM((3, 16, COLS), bf16),
            pltpu.VMEM((2, 1, 32), f32),
            pltpu.VMEM((3, ROWS, COLS), f32),
            pltpu.VMEM((Z, RAW, COLS), bf16),
            pltpu.VMEM((Z, 16, RAW), bf16),
            pltpu.VMEM((Z, 1, META), f32),
            pltpu.VMEM((4, Z, 128), f32),
            pltpu.VMEM((4, Z, 128), f32),
            pltpu.VMEM((3, 1, COLS), f32),
            dma((11,)),
            dma((2, 4, NRAW)), dma((2, 4, NRAW)),
            dma((2, 4, NBLOCK)), dma((2, 4, NBLOCK)),
            dma((2, 4)), dma((2, 4)), dma((2, 4)), dma((2, 4)),
            dma((3,)), dma((3,)), dma((3,)), dma((3,)),
        ],
        compiler_params=pltpu.CompilerParams(
            collective_id=0, has_side_effects=True, vmem_limit_bytes=32 * 1024 * 1024
        ),
    )(tq, lq.T, hq, tk, lk.T, hk, tv, lv.T, hv, nt.reshape(1, 32), ns.reshape(1, 32))
    sq, sk, sv, fq, fk, fv, gain = pl.pallas_call(
        write_kernel,
        name="write_out",
        out_shape=(
            jax.ShapeDtypeStruct((WHOLE, COLS), bf16),
            jax.ShapeDtypeStruct((WHOLE, COLS), bf16),
            jax.ShapeDtypeStruct((WHOLE, COLS), bf16),
            jax.ShapeDtypeStruct((COLS,), f32),
            jax.ShapeDtypeStruct((COLS,), f32),
            jax.ShapeDtypeStruct((COLS,), f32),
            jax.ShapeDtypeStruct((32, 128), bf16),
        ),
        in_specs=[vmem] * 3,
        out_specs=(hbm, hbm, hbm, vmem, vmem, vmem, vmem),
        scratch_shapes=[dma((3,))],
        compiler_params=pltpu.CompilerParams(vmem_limit_bytes=16 * 1024 * 1024),
    )(weights, factors, norm)
    return sq, sk, sv, fq, fk, fv, gain.reshape(4096)


def solution(mesh):
    finer = Mesh(
        mesh.devices.reshape(mesh.shape["zero"], 4, 4, mesh.shape["unit"]),
        ("zero", "width_0", "width_1", "unit"),
    )
    matrix, low, high = P(("unit", "zero"), WIDTH), P(("unit", "zero"), None), P("unit", WIDTH)
    return jax.shard_map(
        per_device,
        mesh=finer,
        in_specs=(matrix, low, high) * 3 + (P(UNIT_ZERO_WIDTH), P(UNIT_ZERO_WIDTH)),
        out_specs=(high, high, high, P(UNIT_WIDTH), P(UNIT_WIDTH), P(UNIT_WIDTH), P("unit")),
        check_vma=False,
    )
```

```python
import functools

import jax
import jax.numpy as jnp
from jax import lax
from jax.experimental import pallas as pl
from jax.experimental.pallas import tpu as pltpu
from jax.sharding import Mesh
from jax.sharding import PartitionSpec as P

WIDTH = ("width_0", "width_1")
UNIT_ZERO_WIDTH = ("unit", "zero", "width_0", "width_1")
UNIT_WIDTH = ("unit", "width_0", "width_1")
MESH = pl.DeviceIdType.MESH

mix_rate = 1.0

Z = 8
ROWS = 512
COLS = 256
WHOLE = Z * ROWS
BLOCK = 128
NRAW = ROWS // BLOCK
PIECE = 256
NPIECE = 2 * ROWS // PIECE
META = 3 * COLS + 128


def fresh_of(low_t, high, train):
    product = lax.dot_general(
        low_t, high, (((0,), (0,)), ((), ())), preferred_element_type=jnp.float32
    )
    return train.astype(jnp.float32) + mix_rate * product


def gather_kernel(
    tq, lq, hq, tk, lk, hk, tv, lv, hv, nt, ns,
    out, factor_q, factor_k, factor_v, norm,
    train, low, high, norm_in, fresh, rawx, lowx, meta, norm_x, norm_y, norm_all, inverse,
    load_sem, raw_s, raw_r, piece_s, piece_r, meta_s, meta_r, low_s, low_r,
    lx_s, lx_r, nx_s, nx_r, ny_s, ny_r,
):
    z = lax.axis_index("zero")
    y = lax.axis_index("width_0")
    x = lax.axis_index("width_1")

    lanes = pl.ds(pl.multiple_of(x * BLOCK, BLOCK), BLOCK)
    loads = [
        pltpu.make_async_copy(src, dst, load_sem.at[n])
        for n, (src, dst) in enumerate((
            (tq, train.at[0]), (lq.at[:, lanes], lowx.at[x, z]), (lq, low.at[0]), (hq, high.at[0]),
            (tk, train.at[1]), (lk, low.at[1]), (hk, high.at[1]),
            (tv, train.at[2]), (lv, low.at[2]), (hv, high.at[2]),
            (nt, norm_in.at[0]), (ns, norm_in.at[1]),
        ))
    ]
    for load in loads:
        load.start()

    def beside(axis, at, step, size):
        return {axis: lax.rem(at + (step + size), size)}

    towards = (beside("zero", z, 1, Z), beside("zero", z, -1, Z))
    barrier = pltpu.get_barrier_semaphore()
    neighbours = towards + (
        beside("width_0", y, 1, 4), beside("width_0", y, -1, 4),
        beside("width_1", x, 1, 4), beside("width_1", x, -1, 4),
    )
    for neighbour in neighbours:
        pl.semaphore_signal(barrier, inc=1, device_id=neighbour, device_id_type=MESH)
    pl.semaphore_wait(barrier, len(neighbours))

    def origin(d, h):
        back = h - 1
        return lax.rem(z + (Z - back if d == 0 else back), Z)

    def remote(src, dst, send, recv, d):
        return pltpu.make_async_remote_copy(
            src_ref=src, dst_ref=dst, send_sem=send, recv_sem=recv,
            device_id=towards[d], device_id_type=MESH,
        )

    def half(start, size, d, h):
        return (start, size) if h < 4 else (start + d * (size // 2), size // 2)

    def raw_copy(d, h, c):
        at, size = half(c * BLOCK, BLOCK, d, h)
        there = rawx.at[origin(d, h), pl.ds(at, size)]
        here = train.at[0, pl.ds(at, size)] if h == 1 else there
        return remote(here, there, raw_s.at[d, h - 1, c], raw_r.at[d, h - 1, c], d)

    def low_copy(d, h):
        ref = lowx.at[x, origin(d, h)]
        return remote(ref, ref, low_s.at[d, h - 1], low_r.at[d, h - 1], d)

    def meta_copy(d, h):
        ref = meta.at[origin(d, h)]
        return remote(ref, ref, meta_s.at[d, h - 1], meta_r.at[d, h - 1], d)

    def row_of(m, r, o):
        return m * WHOLE + o * ROWS + r

    def piece_copy(d, h, j):
        m, r = 1 + j * PIECE // ROWS, j * PIECE % ROWS
        at, size = half(row_of(m, r, origin(d, h)), PIECE, d, h)
        ref = out.at[pl.ds(pl.multiple_of(at, size), size)]
        return remote(ref, ref, piece_s.at[d, h - 1, j], piece_r.at[d, h - 1, j], d)

    def copies(kind, n, h):
        if kind == "meta":
            return [meta_copy(d, h) for d in ((0, 1) if h < 4 else (0,))]
        if kind == "low":
            return [low_copy(d, h) for d in ((0, 1) if h < 4 else (1,))]
        return [(raw_copy if kind == "raw" else piece_copy)(d, h, n) for d in (0, 1)]

    sent, landed = [], set()

    def arrived(*item):
        if item not in landed:
            landed.add(item)
            for copy in copies(*item):
                copy.wait_recv()

    def send(*items):
        for kind, n, h in items:
            if h > 1:
                arrived(kind, n, h - 1)
            for copy in copies(kind, n, h):
                copy.start()
            sent.append((kind, n, h))

    def raw(h, *pieces):
        return [("raw", c, h) for c in pieces]

    def small(h):
        return [("low", 0, h), ("meta", 0, h)]

    loads[0].wait()
    loads[1].wait()
    send(("raw", 0, 1), ("low", 0, 1), ("raw", 1, 1))
    for load in loads[2:]:
        load.wait()
    for m in range(3):
        top = jnp.zeros((8, COLS), jnp.float32)
        for b in range(ROWS // BLOCK):
            rows = pl.ds(b * BLOCK, BLOCK)
            block = fresh_of(low[m, :, rows], high[m], train[m, rows])
            fresh[m, rows] = block
            top = jnp.maximum(top, jnp.max(jnp.abs(block).reshape(BLOCK // 8, 8, COLS), axis=0))
        meta[z, :, pl.ds(m * COLS, COLS)] = jnp.max(top, axis=0, keepdims=True)
    gain = (norm_in[0] + norm_in[1]).astype(jnp.bfloat16)
    lane = lax.broadcasted_iota(jnp.int32, (32, 128), 1)
    entry = lax.broadcasted_iota(jnp.int32, (32, 128), 0)
    place = (lane == entry + 32 * x).astype(jnp.bfloat16)
    meta[z, :, pl.ds(3 * COLS, 128)] = jnp.dot(gain, place, preferred_element_type=jnp.float32)

    send(("meta", 0, 1), *raw(1, 2, 3))
    send(*small(2), *raw(2, 0, 1))
    send(*small(3), *raw(2, 2, 3))
    send(*small(4), *raw(3, 0, 1, 2, 3))
    arrived("meta", 0, 4)

    top = jnp.max(meta[:, 0, : 3 * COLS], axis=0, keepdims=True)
    for m, factor in enumerate((factor_q, factor_k, factor_v)):
        of_m = top[:, m * COLS : (m + 1) * COLS]
        factor[...] = of_m[0]
        inverse[m] = 1.0 / of_m

    def scale_own(m, r, size):
        scaled = fresh[m, pl.ds(r, size)] * inverse[m]
        at = pl.multiple_of(row_of(m, r, z), size)
        out[pl.ds(at, size)] = scaled.astype(jnp.bfloat16)

    for j in range(NPIECE):
        scale_own(1 + j * PIECE // ROWS, j * PIECE % ROWS, PIECE)
        if j > 0:
            send(("piece", j - 1, 1))
    scale_own(0, 0, ROWS)
    send(("piece", NPIECE - 1, 1))

    def hop(n, buf, at, axis, send_sem, recv_sem):
        slot, step = ((at, 1), (at, -1), (lax.rem(at + 3, 4), 1))[n]
        return pltpu.make_async_remote_copy(
            src_ref=buf.at[slot], dst_ref=buf.at[slot], send_sem=send_sem.at[n],
            recv_sem=recv_sem.at[n], device_id=beside(axis, at, step, 4), device_id_type=MESH,
        )

    low_x = (lowx, x, "width_1", lx_s, lx_r)
    gain_x = (norm_x, x, "width_1", nx_s, nx_r)
    gain_y = (norm_y, y, "width_0", ny_s, ny_r)

    def begin(*ring):
        hop(0, *ring).start()
        hop(1, *ring).start()

    def pass_on(*ring):
        hop(0, *ring).wait_recv()
        hop(2, *ring).start()
        hop(1, *ring).wait_recv()

    arrived("low", 0, 4)
    norm_x[x] = meta[:, 0, 3 * COLS :]
    begin(*low_x)
    begin(*gain_x)

    def scale_raw(back):
        o = lax.rem(z + back, Z)
        for b in range(NRAW):
            rows = pl.ds(b * BLOCK, BLOCK)
            block = fresh_of(lowx[b, o], high[0], rawx[o, rows])
            at = pl.multiple_of(row_of(0, b * BLOCK, o), BLOCK)
            out[pl.ds(at, BLOCK)] = (block * inverse[0]).astype(jnp.bfloat16)

    send(*raw(4, 0, 1, 2, 3))
    pass_on(*low_x)
    pass_on(*gain_x)
    send(("piece", 0, 2), ("piece", 1, 2))
    hop(2, *low_x).wait_recv()
    hop(2, *gain_x).wait_recv()
    norm_y[y] = jnp.sum(norm_x[...], axis=0)
    begin(*gain_y)
    scale_raw(1)
    scale_raw(7)
    send(("piece", 2, 2))
    pass_on(*gain_y)
    scale_raw(2)
    scale_raw(6)
    send(("piece", 3, 2))
    scale_raw(3)
    scale_raw(5)
    hop(2, *gain_y).wait_recv()
    for s in range(4):
        for t in range(Z):
            norm_all[pl.ds(t * 4 + s, 1)] = norm_y[s, pl.ds(t, 1)]
    norm[...] = norm_all[...].astype(jnp.bfloat16)
    send(("piece", 0, 3))
    for c in range(NRAW):
        arrived("raw", c, 4)
    scale_raw(4)
    send(*[("piece", j, 3) for j in range(1, NPIECE)])
    send(*[("piece", j, 4) for j in range(NPIECE)])
    for j in range(NPIECE):
        arrived("piece", j, 4)

    for item in sent:
        for copy in copies(*item):
            copy.wait_send()
    for ring in (low_x, gain_x, gain_y):
        for n in range(3):
            hop(n, *ring).wait_send()


def write_kernel(weights, fq, fk, fv, gain, sq, sk, sv, oq, ok, ov, og, sem):
    writes = [
        pltpu.make_async_copy(src, dst, sem.at[n])
        for n, (src, dst) in enumerate((
            (weights.at[pl.ds(0, WHOLE)], sq), (weights.at[pl.ds(WHOLE, WHOLE)], sk),
            (weights.at[pl.ds(2 * WHOLE, WHOLE)], sv), (fq, oq), (fk, ok), (fv, ov), (gain, og),
        ))
    ]
    for write in writes:
        write.start()
    for write in writes:
        write.wait()


def per_device(tq, lq, hq, tk, lk, hk, tv, lv, hv, nt, ns):
    hbm = pl.BlockSpec(memory_space=pltpu.HBM)
    vmem = pl.BlockSpec(memory_space=pltpu.VMEM)
    dma = pltpu.SemaphoreType.DMA
    f32, bf16 = jnp.float32, jnp.bfloat16
    args = (tq, lq.T, hq, tk, lk.T, hk, tv, lv.T, hv, nt.reshape(1, 32), ns.reshape(1, 32))
    gathered = pl.pallas_call(
        gather_kernel,
        name="gather_z",
        out_shape=(pltpu.VMEM((3 * WHOLE, COLS), bf16),)
        + (pltpu.VMEM((COLS,), f32),) * 3
        + (pltpu.VMEM((32, 128), bf16),),
        in_specs=[hbm] * 11,
        out_specs=(vmem,) * 5,
        scratch_shapes=[
            pltpu.VMEM((3, ROWS, COLS), bf16),
            pltpu.VMEM((3, 16, ROWS), bf16),
            pltpu.VMEM((3, 16, COLS), bf16),
            pltpu.VMEM((2, 1, 32), f32),
            pltpu.VMEM((3, ROWS, COLS), f32),
            pltpu.VMEM((Z, ROWS, COLS), bf16),
            pltpu.VMEM((4, Z, 16, BLOCK), bf16),
            pltpu.VMEM((Z, 1, META), f32),
            pltpu.VMEM((4, Z, 128), f32),
            pltpu.VMEM((4, Z, 128), f32),
            pltpu.VMEM((32, 128), f32),
            pltpu.VMEM((3, 1, COLS), f32),
            dma((12,)),
            dma((2, 4, NRAW)), dma((2, 4, NRAW)),
            dma((2, 4, NPIECE)), dma((2, 4, NPIECE)),
            dma((2, 4)), dma((2, 4)), dma((2, 4)), dma((2, 4)),
            dma((3,)), dma((3,)), dma((3,)), dma((3,)), dma((3,)), dma((3,)),
        ],
        compiler_params=pltpu.CompilerParams(
            collective_id=0, has_side_effects=True, vmem_limit_bytes=32 * 1024 * 1024
        ),
    )(*[pltpu.with_memory_space_constraint(a, pltpu.HBM) for a in args])
    shapes = ((WHOLE, COLS), bf16), ((COLS,), f32)
    sq, sk, sv, fq, fk, fv, gain = pl.pallas_call(
        write_kernel,
        name="write_out",
        out_shape=(jax.ShapeDtypeStruct(*shapes[0]),) * 3
        + (jax.ShapeDtypeStruct(*shapes[1]),) * 3
        + (jax.ShapeDtypeStruct((32, 128), bf16),),
        in_specs=[vmem] * 5,
        out_specs=(hbm,) * 7,
        scratch_shapes=[dma((7,))],
        compiler_params=pltpu.CompilerParams(vmem_limit_bytes=16 * 1024 * 1024),
    )(*gathered)
    return sq, sk, sv, fq, fk, fv, gain.reshape(4096)


def solution(mesh):
    finer = Mesh(
        mesh.devices.reshape(mesh.shape["zero"], 4, 4, mesh.shape["unit"]),
        ("zero", "width_0", "width_1", "unit"),
    )
    matrix, low, high = P(("unit", "zero"), WIDTH), P(("unit", "zero"), None), P("unit", WIDTH)
    return jax.shard_map(
        per_device,
        mesh=finer,
        in_specs=(matrix, low, high) * 3 + (P(UNIT_ZERO_WIDTH), P(UNIT_ZERO_WIDTH)),
        out_specs=(high, high, high, P(UNIT_WIDTH), P(UNIT_WIDTH), P(UNIT_WIDTH), P("unit")),
        check_vma=False,
    )
```

```python
import functools

import jax
import jax.numpy as jnp
from jax import lax
from jax.experimental import pallas as pl
from jax.experimental.pallas import tpu as pltpu
from jax.sharding import Mesh
from jax.sharding import PartitionSpec as P

WIDTH = ("width_0", "width_1")
UNIT_ZERO_WIDTH = ("unit", "zero", "width_0", "width_1")
UNIT_WIDTH = ("unit", "width_0", "width_1")
MESH = pl.DeviceIdType.MESH

mix_rate = 1.0

Z = 8
ROWS = 512
COLS = 256
WHOLE = Z * ROWS
BLOCK = 128
NBLOCK = ROWS // BLOCK
PIECE = 256
NPIECE = 2 * ROWS // PIECE
META = 3 * COLS + 128


def fresh_of(low_t, high, train):
    product = lax.dot_general(
        low_t, high, (((0,), (0,)), ((), ())), preferred_element_type=jnp.float32
    )
    return train.astype(jnp.float32) + mix_rate * product


def gather_kernel(
    tq, lq, hq, tk, lk, hk, tv, lv, hv, nt, ns,
    out, factor_q, factor_k, factor_v, norm,
    train, low, high, norm_in, fresh, rawx, lowx, meta, norm_x, norm_y, norm_all, inverse,
    load_sem, raw_s, raw_r, piece_s, piece_r, meta_s, meta_r, low_s, low_r,
    lx_s, lx_r, nx_s, nx_r, ny_s, ny_r, ready,
):
    z = lax.axis_index("zero")
    y = lax.axis_index("width_0")
    x = lax.axis_index("width_1")

    lanes = pl.ds(pl.multiple_of(x * BLOCK, BLOCK), BLOCK)
    loads = [
        pltpu.make_async_copy(src, dst, load_sem.at[n])
        for n, (src, dst) in enumerate((
            (tq, train.at[0]), (lq.at[:, lanes], lowx.at[x, z]), (lq, low.at[0]), (hq, high.at[0]),
            (tk, train.at[1]), (lk, low.at[1]), (hk, high.at[1]),
            (tv, train.at[2]), (lv, low.at[2]), (hv, high.at[2]),
            (nt, norm_in.at[0]), (ns, norm_in.at[1]),
        ))
    ]
    for load in loads:
        load.start()

    def beside(axis, at, step, size):
        return {axis: lax.rem(at + (step + size), size)}

    towards = (beside("zero", z, 1, Z), beside("zero", z, -1, Z))
    barrier = pltpu.get_barrier_semaphore()
    for neighbour in towards:
        pl.semaphore_signal(barrier, inc=1, device_id=neighbour, device_id_type=MESH)
    plane = (("width_1", x), ("width_0", y))
    for axis, at in plane:
        @pl.when(at < 3)
        def _(axis=axis, at=at):
            pl.semaphore_signal(barrier, inc=1, device_id={axis: lax.rem(at + 1, 4)}, device_id_type=MESH)

        @pl.when(at == 0)
        def _(axis=axis, at=at):
            pl.semaphore_signal(barrier, inc=1, device_id={axis: lax.rem(at + 3, 4)}, device_id_type=MESH)

    lower = [(at + 1) // 2 for _, at in plane]
    pl.semaphore_wait(barrier, 2 + lower[0] + lower[1])

    def answer():
        for n, (axis, at) in enumerate(plane):
            @pl.when(at > 0)
            def _(n=n, axis=axis, at=at):
                pl.semaphore_signal(ready.at[n], inc=1, device_id={axis: lax.rem(at + 3, 4)}, device_id_type=MESH)

            @pl.when(at == 3)
            def _(n=n, axis=axis, at=at):
                pl.semaphore_signal(ready.at[n], inc=1, device_id={axis: lax.rem(at + 1, 4)}, device_id_type=MESH)

    def origin(d, h):
        back = h - 1
        return lax.rem(z + (Z - back if d == 0 else back), Z)

    def remote(src, dst, send, recv, d):
        return pltpu.make_async_remote_copy(
            src_ref=src, dst_ref=dst, send_sem=send, recv_sem=recv,
            device_id=towards[d], device_id_type=MESH,
        )

    def raw_copy(d, h, n):
        size = BLOCK if h < 3 else 2 * BLOCK
        rows = pl.ds((n if h < 4 else d) * size, size)
        there = rawx.at[origin(d, h), rows]
        here = train.at[0, rows] if h == 1 else there
        return remote(here, there, raw_s.at[d, h - 1, n], raw_r.at[d, h - 1, n], d)

    def low_copy(d, h, n):
        ref = lowx.at[x, origin(d, h)]
        return remote(ref, ref, low_s.at[d, h - 1], low_r.at[d, h - 1], d)

    def meta_copy(d, h, n):
        ref = meta.at[origin(d, h)]
        return remote(ref, ref, meta_s.at[d, h - 1], meta_r.at[d, h - 1], d)

    def row_of(m, r, o):
        return m * WHOLE + o * ROWS + r

    def piece_copy(d, h, n):
        m, r = 1 + n * PIECE // ROWS, n * PIECE % ROWS
        ref = out.at[pl.ds(pl.multiple_of(row_of(m, r, origin(d, h)), PIECE), PIECE)]
        return remote(ref, ref, piece_s.at[d, h - 1, n], piece_r.at[d, h - 1, n], d)

    copy_of = {"raw": raw_copy, "low": low_copy, "meta": meta_copy, "piece": piece_copy}

    def goes(kind, n, h, d):
        if h < 4 or kind == "raw":
            return True
        return {"low": d == 1, "meta": d == 0, "piece": n * 2 // NPIECE == d}[kind]

    def needs(kind, n, h, d):
        if h == 1:
            return []
        if kind == "raw" and h > 2:
            return [(kind, 2 * n, 2), (kind, 2 * n + 1, 2)] if h == 3 else [(kind, d, 3)]
        return [(kind, n, h - 1)]

    sent, landed = [], set()

    def arrived_one(kind, n, h, d):
        if goes(kind, n, h, d) and (kind, n, h, d) not in landed:
            landed.add((kind, n, h, d))
            copy_of[kind](d, h, n).wait_recv()

    def arrived(*item):
        for d in (0, 1):
            arrived_one(*item, d)

    def send(*items):
        for kind, n, h in items:
            for d in (0, 1):
                if goes(kind, n, h, d):
                    for before in needs(kind, n, h, d):
                        arrived_one(*before, d)
                    copy_of[kind](d, h, n).start()
                    sent.append((kind, n, h, d))

    def raw(h, *pieces):
        return [("raw", n, h) for n in pieces]

    def small(h):
        return [("low", 0, h), ("meta", 0, h)]

    loads[0].wait()
    loads[1].wait()
    send(("raw", 0, 1), ("low", 0, 1))
    answer()
    for load in loads[2:]:
        load.wait()
    for m in range(3):
        top = jnp.zeros((8, COLS), jnp.float32)
        for b in range(ROWS // BLOCK):
            rows = pl.ds(b * BLOCK, BLOCK)
            block = fresh_of(low[m, :, rows], high[m], train[m, rows])
            fresh[m, rows] = block
            top = jnp.maximum(top, jnp.max(jnp.abs(block).reshape(BLOCK // 8, 8, COLS), axis=0))
        meta[z, :, pl.ds(m * COLS, COLS)] = jnp.max(top, axis=0, keepdims=True)
    gain = (norm_in[0] + norm_in[1]).astype(jnp.bfloat16)
    lane = lax.broadcasted_iota(jnp.int32, (32, 128), 1)
    entry = lax.broadcasted_iota(jnp.int32, (32, 128), 0)
    place = (lane == entry + 32 * x).astype(jnp.bfloat16)
    meta[z, :, pl.ds(3 * COLS, 128)] = jnp.dot(gain, place, preferred_element_type=jnp.float32)

    send(("meta", 0, 1), *raw(1, 1, 2))
    send(*small(2), *raw(1, 3), *raw(2, 0))
    send(*small(3), *raw(2, 1, 2))
    send(*small(4), *raw(2, 3), *raw(3, 0))
    arrived("meta", 0, 3)
    arrived("meta", 0, 4)

    top = jnp.max(meta[:, 0, : 3 * COLS], axis=0, keepdims=True)
    for m, factor in enumerate((factor_q, factor_k, factor_v)):
        of_m = top[:, m * COLS : (m + 1) * COLS]
        factor[...] = of_m[0]
        inverse[m] = 1.0 / of_m

    def scale_own(m, r, size):
        scaled = fresh[m, pl.ds(r, size)] * inverse[m]
        at = pl.multiple_of(row_of(m, r, z), size)
        out[pl.ds(at, size)] = scaled.astype(jnp.bfloat16)

    for j in range(NPIECE):
        scale_own(1 + j * PIECE // ROWS, j * PIECE % ROWS, PIECE)
        if j > 0:
            send(("piece", j - 1, 1))
    scale_own(0, 0, ROWS)
    send(("piece", NPIECE - 1, 1), *raw(3, 1))

    def hop(n, buf, at, axis, send_sem, recv_sem):
        slot, step = ((at, 1), (at, -1), (lax.rem(at + 3, 4), 1))[n]
        return pltpu.make_async_remote_copy(
            src_ref=buf.at[slot], dst_ref=buf.at[slot], send_sem=send_sem.at[n],
            recv_sem=recv_sem.at[n], device_id=beside(axis, at, step, 4), device_id_type=MESH,
        )

    low_x = (lowx, x, "width_1", lx_s, lx_r)
    gain_x = (norm_x, x, "width_1", nx_s, nx_r)
    gain_y = (norm_y, y, "width_0", ny_s, ny_r)

    def begin(*ring):
        hop(0, *ring).start()
        hop(1, *ring).start()

    def pass_on(*ring):
        hop(0, *ring).wait_recv()
        hop(2, *ring).start()
        hop(1, *ring).wait_recv()

    arrived("low", 0, 3)
    arrived("low", 0, 4)
    norm_x[x] = meta[:, 0, 3 * COLS :]
    for n, (_, at) in enumerate(plane):
        @pl.when(at < 3)
        def _(n=n):
            pl.semaphore_wait(ready.at[n], 2 - lower[n])
    begin(*low_x)
    begin(*gain_x)

    def scale_raw(back):
        o = lax.rem(z + back, Z)
        for b in range(NBLOCK):
            rows = pl.ds(b * BLOCK, BLOCK)
            block = fresh_of(lowx[b, o], high[0], rawx[o, rows])
            at = pl.multiple_of(row_of(0, b * BLOCK, o), BLOCK)
            out[pl.ds(at, BLOCK)] = (block * inverse[0]).astype(jnp.bfloat16)

    send(*raw(4, 0))
    pass_on(*low_x)
    pass_on(*gain_x)
    send(("piece", 0, 2), ("piece", 1, 2))
    hop(2, *low_x).wait_recv()
    hop(2, *gain_x).wait_recv()
    norm_y[y] = jnp.sum(norm_x[...], axis=0)
    begin(*gain_y)
    scale_raw(1)
    scale_raw(7)
    send(("piece", 2, 2))
    pass_on(*gain_y)
    scale_raw(2)
    scale_raw(6)
    send(("piece", 3, 2))
    arrived("raw", 0, 3)
    arrived("raw", 1, 3)
    scale_raw(3)
    scale_raw(5)
    hop(2, *gain_y).wait_recv()
    for s in range(4):
        for t in range(Z):
            norm_all[pl.ds(t * 4 + s, 1)] = norm_y[s, pl.ds(t, 1)]
    norm[...] = norm_all[...].astype(jnp.bfloat16)
    send(("piece", 0, 3))
    arrived("raw", 0, 4)
    scale_raw(4)
    send(*[("piece", n, 3) for n in range(1, NPIECE)])
    send(*[("piece", n, 4) for n in range(NPIECE)])
    for n in range(NPIECE):
        arrived("piece", n, 3)
    for n in range(NPIECE):
        arrived("piece", n, 4)

    for kind, n, h, d in sent:
        copy_of[kind](d, h, n).wait_send()
    for ring in (low_x, gain_x, gain_y):
        for n in range(3):
            hop(n, *ring).wait_send()


def write_kernel(weights, fq, fk, fv, gain, sq, sk, sv, oq, ok, ov, og, sem):
    writes = [
        pltpu.make_async_copy(src, dst, sem.at[n])
        for n, (src, dst) in enumerate((
            (weights.at[pl.ds(0, WHOLE)], sq), (weights.at[pl.ds(WHOLE, WHOLE)], sk),
            (weights.at[pl.ds(2 * WHOLE, WHOLE)], sv), (fq, oq), (fk, ok), (fv, ov), (gain, og),
        ))
    ]
    for write in writes:
        write.start()
    for write in writes:
        write.wait()


def per_device(tq, lq, hq, tk, lk, hk, tv, lv, hv, nt, ns):
    hbm = pl.BlockSpec(memory_space=pltpu.HBM)
    vmem = pl.BlockSpec(memory_space=pltpu.VMEM)
    dma = pltpu.SemaphoreType.DMA
    f32, bf16 = jnp.float32, jnp.bfloat16
    args = (tq, lq.T, hq, tk, lk.T, hk, tv, lv.T, hv, nt.reshape(1, 32), ns.reshape(1, 32))
    gathered = pl.pallas_call(
        gather_kernel,
        name="gather_z",
        out_shape=(pltpu.VMEM((3 * WHOLE, COLS), bf16),)
        + (pltpu.VMEM((COLS,), f32),) * 3
        + (pltpu.VMEM((32, 128), bf16),),
        in_specs=[hbm] * 11,
        out_specs=(vmem,) * 5,
        scratch_shapes=[
            pltpu.VMEM((3, ROWS, COLS), bf16),
            pltpu.VMEM((3, 16, ROWS), bf16),
            pltpu.VMEM((3, 16, COLS), bf16),
            pltpu.VMEM((2, 1, 32), f32),
            pltpu.VMEM((3, ROWS, COLS), f32),
            pltpu.VMEM((Z, ROWS, COLS), bf16),
            pltpu.VMEM((4, Z, 16, BLOCK), bf16),
            pltpu.VMEM((Z, 1, META), f32),
            pltpu.VMEM((4, Z, 128), f32),
            pltpu.VMEM((4, Z, 128), f32),
            pltpu.VMEM((32, 128), f32),
            pltpu.VMEM((3, 1, COLS), f32),
            dma((12,)),
            dma((2, 4, NBLOCK)), dma((2, 4, NBLOCK)),
            dma((2, 4, NPIECE)), dma((2, 4, NPIECE)),
            dma((2, 4)), dma((2, 4)), dma((2, 4)), dma((2, 4)),
            dma((3,)), dma((3,)), dma((3,)), dma((3,)), dma((3,)), dma((3,)),
            pltpu.SemaphoreType.REGULAR((2,)),
        ],
        compiler_params=pltpu.CompilerParams(
            collective_id=0, has_side_effects=True, vmem_limit_bytes=32 * 1024 * 1024
        ),
    )(*[pltpu.with_memory_space_constraint(a, pltpu.HBM) for a in args])
    shapes = ((WHOLE, COLS), bf16), ((COLS,), f32)
    sq, sk, sv, fq, fk, fv, gain = pl.pallas_call(
        write_kernel,
        name="write_out",
        out_shape=(jax.ShapeDtypeStruct(*shapes[0]),) * 3
        + (jax.ShapeDtypeStruct(*shapes[1]),) * 3
        + (jax.ShapeDtypeStruct((32, 128), bf16),),
        in_specs=[vmem] * 5,
        out_specs=(hbm,) * 7,
        scratch_shapes=[dma((7,))],
        compiler_params=pltpu.CompilerParams(vmem_limit_bytes=16 * 1024 * 1024),
    )(*gathered)
    return sq, sk, sv, fq, fk, fv, gain.reshape(4096)


def solution(mesh):
    finer = Mesh(
        mesh.devices.reshape(mesh.shape["zero"], 4, 4, mesh.shape["unit"]),
        ("zero", "width_0", "width_1", "unit"),
    )
    matrix, low, high = P(("unit", "zero"), WIDTH), P(("unit", "zero"), None), P("unit", WIDTH)
    return jax.shard_map(
        per_device,
        mesh=finer,
        in_specs=(matrix, low, high) * 3 + (P(UNIT_ZERO_WIDTH), P(UNIT_ZERO_WIDTH)),
        out_specs=(high, high, high, P(UNIT_WIDTH), P(UNIT_WIDTH), P(UNIT_WIDTH), P("unit")),
        check_vma=False,
    )
```

```python
import functools

import jax
import jax.numpy as jnp
from jax import lax
from jax.experimental import pallas as pl
from jax.experimental.pallas import tpu as pltpu
from jax.sharding import Mesh
from jax.sharding import PartitionSpec as P

WIDTH = ("width_0", "width_1")
UNIT_ZERO_WIDTH = ("unit", "zero", "width_0", "width_1")
UNIT_WIDTH = ("unit", "width_0", "width_1")
MESH = pl.DeviceIdType.MESH

mix_rate = 1.0

Z = 8
ROWS = 512
COLS = 256
WHOLE = Z * ROWS
BLOCK = 128
NBLOCK = ROWS // BLOCK
PIECE = 256
NPIECE = 2 * ROWS // PIECE
META = 3 * COLS + 128
RAW, SCALED, LOW, TOP, LOW_X, NORM_X, NORM_Y = range(7)


def fresh_of(low_t, high, train):
    product = lax.dot_general(
        low_t, high, (((0,), (0,)), ((), ())), preferred_element_type=jnp.float32
    )
    return train.astype(jnp.float32) + mix_rate * product


def gather_kernel(
    tq, lq, hq, tk, lk, hk, tv, lv, hv, nt, ns,
    out, factor_q, factor_k, factor_v, norm,
    train, low, high, norm_in, fresh, rawx, lowx, meta, norm_x, norm_y, norm_all, inverse,
    load_sem, sends, raw_r, piece_r, meta_r, low_r, last, lx_r, nx_r, ny_r, ready,
):
    z = lax.axis_index("zero")
    y = lax.axis_index("width_0")
    x = lax.axis_index("width_1")

    lanes = pl.ds(pl.multiple_of(x * BLOCK, BLOCK), BLOCK)
    groups = (
        ((tq, train.at[0]),),
        ((lq.at[:, lanes], lowx.at[x, z]),),
        ((tk, train.at[1]), (tv, train.at[2])),
        ((lq, low.at[0]), (lk, low.at[1]), (lv, low.at[2])),
        ((hq, high.at[0]), (hk, high.at[1]), (hv, high.at[2])),
        ((nt, norm_in.at[0]), (ns, norm_in.at[1])),
    )
    for n, group in enumerate(groups):
        for src, dst in group:
            pltpu.make_async_copy(src, dst, load_sem.at[n]).start()

    def all_of(ref, sem):
        pltpu.make_async_copy(ref, ref, sem).wait()

    def beside(axis, at, step, size):
        return {axis: lax.rem(at + (step + size), size)}

    towards = (beside("zero", z, 1, Z), beside("zero", z, -1, Z))
    barrier = pltpu.get_barrier_semaphore()
    for neighbour in towards:
        pl.semaphore_signal(barrier, inc=1, device_id=neighbour, device_id_type=MESH)
    plane = (("width_1", x), ("width_0", y))
    for axis, at in plane:
        @pl.when(at < 3)
        def _(axis=axis, at=at):
            pl.semaphore_signal(barrier, inc=1, device_id={axis: lax.rem(at + 1, 4)}, device_id_type=MESH)

        @pl.when(at == 0)
        def _(axis=axis, at=at):
            pl.semaphore_signal(barrier, inc=1, device_id={axis: lax.rem(at + 3, 4)}, device_id_type=MESH)

    lower = [(at + 1) // 2 for _, at in plane]
    pl.semaphore_wait(barrier, 2 + lower[0] + lower[1])

    def answer():
        for n, (axis, at) in enumerate(plane):
            @pl.when(at > 0)
            def _(n=n, axis=axis, at=at):
                pl.semaphore_signal(ready.at[n], inc=1, device_id={axis: lax.rem(at + 3, 4)}, device_id_type=MESH)

            @pl.when(at == 3)
            def _(n=n, axis=axis, at=at):
                pl.semaphore_signal(ready.at[n], inc=1, device_id={axis: lax.rem(at + 1, 4)}, device_id_type=MESH)

    def origin(d, h):
        back = h - 1
        return lax.rem(z + (Z - back if d == 0 else back), Z)

    def remote(src, dst, kind, recv, d):
        return pltpu.make_async_remote_copy(
            src_ref=src, dst_ref=dst, send_sem=sends.at[kind], recv_sem=recv,
            device_id=towards[d], device_id_type=MESH,
        )

    def half(start, size, d, h):
        return (start, size) if h < 4 else (start + d * (size // 2), size // 2)

    def raw_copy(d, h, n):
        at, size = half(n * BLOCK, BLOCK, d, h)
        there = rawx.at[origin(d, h), pl.ds(at, size)]
        here = train.at[0, pl.ds(at, size)] if h == 1 else there
        recv = raw_r.at[d, h - 1, n] if h < 4 else last.at[RAW]
        return remote(here, there, RAW, recv, d)

    def low_copy(d, h, n):
        ref = lowx.at[x, origin(d, h)]
        recv = last.at[LOW] if ends(LOW, d, h) else low_r.at[d, h - 1]
        return remote(ref, ref, LOW, recv, d)

    def meta_copy(d, h, n):
        ref = meta.at[origin(d, h)]
        recv = last.at[TOP] if ends(TOP, d, h) else meta_r.at[1 - d, h - 1]
        return remote(ref, ref, TOP, recv, d)

    def row_of(m, r, o):
        return m * WHOLE + o * ROWS + r

    def piece_copy(d, h, n):
        m, r = 1 + n * PIECE // ROWS, n * PIECE % ROWS
        at, size = half(row_of(m, r, origin(d, h)), PIECE, d, h)
        ref = out.at[pl.ds(pl.multiple_of(at, size), size)]
        recv = piece_r.at[d, h - 1, n] if h < 4 else last.at[SCALED]
        return remote(ref, ref, SCALED, recv, d)

    copy_of = (raw_copy, piece_copy, low_copy, meta_copy)

    def goes(kind, h, d):
        return h < 4 or kind in (RAW, SCALED) or d == (1 if kind == LOW else 0)

    def ends(kind, d, h):
        return not goes(kind, h + 1, d) if h < 4 else True

    landed = set()

    def arrived_one(kind, n, h, d):
        if (kind, n, h, d) not in landed and not ends(kind, d, h):
            landed.add((kind, n, h, d))
            copy_of[kind](d, h, n).wait_recv()

    def send(*items):
        for kind, n, h in items:
            for d in (0, 1):
                if h > 1:
                    arrived_one(kind, n, h - 1, d)
                if goes(kind, h, d):
                    copy_of[kind](d, h, n).start()

    def raw(h, *pieces):
        return [(RAW, n, h) for n in pieces]

    def small(h):
        return [(LOW, 0, h), (TOP, 0, h)]

    all_of(train.at[0], load_sem.at[0])
    all_of(lowx.at[x, z], load_sem.at[1])
    send(*raw(1, 0, 1))
    answer()
    all_of(train.at[pl.ds(1, 2)], load_sem.at[2])
    all_of(low, load_sem.at[3])
    all_of(high, load_sem.at[4])
    all_of(norm_in, load_sem.at[5])
    for m in range(3):
        top = jnp.zeros((8, COLS), jnp.float32)
        for b in range(ROWS // BLOCK):
            rows = pl.ds(b * BLOCK, BLOCK)
            block = fresh_of(low[m, :, rows], high[m], train[m, rows])
            fresh[m, rows] = block
            top = jnp.maximum(top, jnp.max(jnp.abs(block).reshape(BLOCK // 8, 8, COLS), axis=0))
        meta[z, :, pl.ds(m * COLS, COLS)] = jnp.max(top, axis=0, keepdims=True)
    gain = (norm_in[0] + norm_in[1]).astype(jnp.bfloat16)
    lane = lax.broadcasted_iota(jnp.int32, (32, 128), 1)
    entry = lax.broadcasted_iota(jnp.int32, (32, 128), 0)
    place = (lane == entry + 32 * x).astype(jnp.bfloat16)
    meta[z, :, pl.ds(3 * COLS, 128)] = jnp.dot(gain, place, preferred_element_type=jnp.float32)

    send(*small(1), *raw(1, 2, 3), *raw(2, 0))
    send(*small(2), *raw(2, 1, 2))
    send(*small(3), *raw(2, 3), *raw(3, 0, 1))
    send(*small(4), *raw(3, 2, 3), *raw(4, 0))
    all_of(meta.at[pl.ds(0, 2)], last.at[TOP])

    top = jnp.max(meta[:, 0, : 3 * COLS], axis=0, keepdims=True)
    for m, factor in enumerate((factor_q, factor_k, factor_v)):
        of_m = top[:, m * COLS : (m + 1) * COLS]
        factor[...] = of_m[0]
        inverse[m] = 1.0 / of_m

    def scale_own(m, r, size):
        scaled = fresh[m, pl.ds(r, size)] * inverse[m]
        at = pl.multiple_of(row_of(m, r, z), size)
        out[pl.ds(at, size)] = scaled.astype(jnp.bfloat16)

    for j in range(NPIECE):
        scale_own(1 + j * PIECE // ROWS, j * PIECE % ROWS, PIECE)
        if j > 0:
            send((SCALED, j - 1, 1))
    scale_own(0, 0, ROWS)
    send((SCALED, NPIECE - 1, 1))

    def hop(n, buf, at, axis, kind, recv):
        slot, step = ((at, 1), (at, -1), (lax.rem(at + 3, 4), 1))[n]
        return pltpu.make_async_remote_copy(
            src_ref=buf.at[slot], dst_ref=buf.at[slot], send_sem=sends.at[kind],
            recv_sem=recv.at[0 if n == 0 else 1], device_id=beside(axis, at, step, 4), device_id_type=MESH,
        )

    low_x = (lowx, x, "width_1", LOW_X, lx_r)
    gain_x = (norm_x, x, "width_1", NORM_X, nx_r)
    gain_y = (norm_y, y, "width_0", NORM_Y, ny_r)

    def begin(*ring):
        hop(0, *ring).start()
        hop(1, *ring).start()

    def pass_on(*ring):
        hop(0, *ring).wait_recv()
        hop(2, *ring).start()

    def complete(buf, at, axis, kind, recv):
        all_of(buf.at[pl.ds(0, 2)], recv.at[1])

    all_of(lowx.at[0, pl.ds(0, 2)], last.at[LOW])
    norm_x[x] = meta[:, 0, 3 * COLS :]
    for n, (_, at) in enumerate(plane):
        @pl.when(at < 3)
        def _(n=n):
            pl.semaphore_wait(ready.at[n], 2 - lower[n])
    begin(*low_x)
    begin(*gain_x)

    def scale_raw(back):
        o = lax.rem(z + back, Z)
        for b in range(NBLOCK):
            rows = pl.ds(b * BLOCK, BLOCK)
            block = fresh_of(lowx[b, o], high[0], rawx[o, rows])
            at = pl.multiple_of(row_of(0, b * BLOCK, o), BLOCK)
            out[pl.ds(at, BLOCK)] = (block * inverse[0]).astype(jnp.bfloat16)

    send(*raw(4, 1, 2, 3))
    pass_on(*low_x)
    pass_on(*gain_x)
    send((SCALED, 0, 2), (SCALED, 1, 2))
    complete(*low_x)
    complete(*gain_x)
    norm_y[y] = jnp.sum(norm_x[...], axis=0)
    begin(*gain_y)
    scale_raw(1)
    scale_raw(7)
    send((SCALED, 2, 2))
    pass_on(*gain_y)
    scale_raw(2)
    scale_raw(6)
    send((SCALED, 3, 2))
    scale_raw(3)
    scale_raw(5)
    complete(*gain_y)
    for s in range(4):
        for t in range(Z):
            norm_all[pl.ds(t * 4 + s, 1)] = norm_y[s, pl.ds(t, 1)]
    norm[...] = norm_all[...].astype(jnp.bfloat16)
    send((SCALED, 0, 3))
    all_of(rawx.at[0], last.at[RAW])
    scale_raw(4)
    send(*[(SCALED, n, 3) for n in range(1, NPIECE)])
    send(*[(SCALED, n, 4) for n in range(NPIECE)])
    all_of(out.at[pl.ds(0, 2 * ROWS)], last.at[SCALED])

    all_of(out.at[pl.ds(0, 7 * ROWS)], sends.at[RAW])
    all_of(out.at[pl.ds(0, 14 * ROWS)], sends.at[SCALED])
    all_of(lowx.at[0, pl.ds(0, 7)], sends.at[LOW])
    all_of(meta.at[pl.ds(0, 7)], sends.at[TOP])
    all_of(lowx.at[pl.ds(0, 3)], sends.at[LOW_X])
    all_of(norm_x.at[pl.ds(0, 3)], sends.at[NORM_X])
    all_of(norm_y.at[pl.ds(0, 3)], sends.at[NORM_Y])


def write_kernel(weights, fq, fk, fv, gain, sq, sk, sv, oq, ok, ov, og, sem):
    writes = [
        pltpu.make_async_copy(src, dst, sem.at[n])
        for n, (src, dst) in enumerate((
            (weights.at[pl.ds(0, WHOLE)], sq), (weights.at[pl.ds(WHOLE, WHOLE)], sk),
            (weights.at[pl.ds(2 * WHOLE, WHOLE)], sv), (fq, oq), (fk, ok), (fv, ov), (gain, og),
        ))
    ]
    for write in writes:
        write.start()
    for write in writes:
        write.wait()


def per_device(tq, lq, hq, tk, lk, hk, tv, lv, hv, nt, ns):
    hbm = pl.BlockSpec(memory_space=pltpu.HBM)
    vmem = pl.BlockSpec(memory_space=pltpu.VMEM)
    dma = pltpu.SemaphoreType.DMA
    f32, bf16 = jnp.float32, jnp.bfloat16
    args = (tq, lq.T, hq, tk, lk.T, hk, tv, lv.T, hv, nt.reshape(1, 32), ns.reshape(1, 32))
    gathered = pl.pallas_call(
        gather_kernel,
        name="gather_z",
        out_shape=(pltpu.VMEM((3 * WHOLE, COLS), bf16),)
        + (pltpu.VMEM((COLS,), f32),) * 3
        + (pltpu.VMEM((32, 128), bf16),),
        in_specs=[hbm] * 11,
        out_specs=(vmem,) * 5,
        scratch_shapes=[
            pltpu.VMEM((3, ROWS, COLS), bf16),
            pltpu.VMEM((3, 16, ROWS), bf16),
            pltpu.VMEM((3, 16, COLS), bf16),
            pltpu.VMEM((2, 1, 32), f32),
            pltpu.VMEM((3, ROWS, COLS), f32),
            pltpu.VMEM((Z, ROWS, COLS), bf16),
            pltpu.VMEM((4, Z, 16, BLOCK), bf16),
            pltpu.VMEM((Z, 1, META), f32),
            pltpu.VMEM((4, Z, 128), f32),
            pltpu.VMEM((4, Z, 128), f32),
            pltpu.VMEM((32, 128), f32),
            pltpu.VMEM((3, 1, COLS), f32),
            dma((6,)), dma((7,)),
            dma((2, 3, NBLOCK)), dma((2, 3, NPIECE)), dma((2, 3)), dma((2, 3)), dma((4,)),
            dma((2,)), dma((2,)), dma((2,)),
            pltpu.SemaphoreType.REGULAR((2,)),
        ],
        compiler_params=pltpu.CompilerParams(
            collective_id=0, has_side_effects=True, vmem_limit_bytes=32 * 1024 * 1024
        ),
    )(*[pltpu.with_memory_space_constraint(a, pltpu.HBM) for a in args])
    shapes = ((WHOLE, COLS), bf16), ((COLS,), f32)
    sq, sk, sv, fq, fk, fv, gain = pl.pallas_call(
        write_kernel,
        name="write_out",
        out_shape=(jax.ShapeDtypeStruct(*shapes[0]),) * 3
        + (jax.ShapeDtypeStruct(*shapes[1]),) * 3
        + (jax.ShapeDtypeStruct((32, 128), bf16),),
        in_specs=[vmem] * 5,
        out_specs=(hbm,) * 7,
        scratch_shapes=[dma((7,))],
        compiler_params=pltpu.CompilerParams(vmem_limit_bytes=16 * 1024 * 1024),
    )(*gathered)
    return sq, sk, sv, fq, fk, fv, gain.reshape(4096)


def solution(mesh):
    finer = Mesh(
        mesh.devices.reshape(mesh.shape["zero"], 4, 4, mesh.shape["unit"]),
        ("zero", "width_0", "width_1", "unit"),
    )
    matrix, low, high = P(("unit", "zero"), WIDTH), P(("unit", "zero"), None), P("unit", WIDTH)
    return jax.shard_map(
        per_device,
        mesh=finer,
        in_specs=(matrix, low, high) * 3 + (P(UNIT_ZERO_WIDTH), P(UNIT_ZERO_WIDTH)),
        out_specs=(high, high, high, P(UNIT_WIDTH), P(UNIT_WIDTH), P(UNIT_WIDTH), P("unit")),
        check_vma=False,
    )
```

```python
import functools

import jax
import jax.numpy as jnp
from jax import lax
from jax.experimental import pallas as pl
from jax.experimental.pallas import tpu as pltpu
from jax.sharding import Mesh
from jax.sharding import PartitionSpec as P

WIDTH = ("width_0", "width_1")
UNIT_ZERO_WIDTH = ("unit", "zero", "width_0", "width_1")
UNIT_WIDTH = ("unit", "width_0", "width_1")
MESH = pl.DeviceIdType.MESH

mix_rate = 1.0

Z = 8
ROWS = 512
COLS = 256
WHOLE = Z * ROWS
BLOCK = 128
NBLOCK = ROWS // BLOCK
PIECE = 256
NPIECE = 2 * ROWS // PIECE
META = 3 * COLS + 128
RAW, SCALED, LOW, TOP, LOW_X, NORM_X, NORM_Y, MOVED = range(8)


def fresh_of(low_t, high, train):
    product = lax.dot_general(
        low_t, high, (((0,), (0,)), ((), ())), preferred_element_type=jnp.float32
    )
    return train.astype(jnp.float32) + mix_rate * product


def gather_kernel(
    tq, lq, hq, tk, lk, hk, tv, lv, hv, nt, ns,
    out, factor_q, factor_k, factor_v, norm,
    train, low, high, norm_in, fresh, rawx, lowx, meta, norm_x, norm_y, norm_all, inverse,
    load_sem, sends, raw_r, piece_r, meta_r, low_r, last, lx_r, nx_r, ny_r, ready,
):
    z = lax.axis_index("zero")
    y = lax.axis_index("width_0")
    x = lax.axis_index("width_1")

    lanes = pl.ds(pl.multiple_of(x * BLOCK, BLOCK), BLOCK)
    groups = (
        ((tq, train.at[0]),),
        ((lq.at[:, lanes], lowx.at[x, z]),),
        ((tk, train.at[1]), (tv, train.at[2])),
        ((lq, low.at[0]), (lk, low.at[1]), (lv, low.at[2])),
        ((hq, high.at[0]), (hk, high.at[1]), (hv, high.at[2])),
        ((nt, norm_in.at[0]), (ns, norm_in.at[1])),
    )
    for n, group in enumerate(groups):
        for src, dst in group:
            pltpu.make_async_copy(src, dst, load_sem.at[n]).start()

    def all_of(ref, sem):
        pltpu.make_async_copy(ref, ref, sem).wait()

    def beside(axis, at, step, size):
        return {axis: lax.rem(at + (step + size), size)}

    towards = (beside("zero", z, 1, Z), beside("zero", z, -1, Z))
    barrier = pltpu.get_barrier_semaphore()
    pl.semaphore_signal(barrier, inc=1, device_id=towards[1], device_id_type=MESH)

    @pl.when(z < Z - 1)
    def _():
        pl.semaphore_signal(barrier, inc=1, device_id=towards[0], device_id_type=MESH)

    plane = (("width_1", x), ("width_0", y))
    for axis, at in plane:
        @pl.when(at < 3)
        def _(axis=axis, at=at):
            pl.semaphore_signal(barrier, inc=1, device_id={axis: lax.rem(at + 1, 4)}, device_id_type=MESH)

        @pl.when(at == 0)
        def _(axis=axis, at=at):
            pl.semaphore_signal(barrier, inc=1, device_id={axis: lax.rem(at + 3, 4)}, device_id_type=MESH)

    lower = [(at + 1) // 2 for _, at in plane]
    pl.semaphore_wait(barrier, 1 + lax.min(z, 1) + lower[0] + lower[1])

    @pl.when(z == Z - 1)
    def _():
        pl.semaphore_signal(ready.at[2], inc=1, device_id=towards[0], device_id_type=MESH)

    def answer():
        for n, (axis, at) in enumerate(plane):
            @pl.when(at > 0)
            def _(n=n, axis=axis, at=at):
                pl.semaphore_signal(ready.at[n], inc=1, device_id={axis: lax.rem(at + 3, 4)}, device_id_type=MESH)

            @pl.when(at == 3)
            def _(n=n, axis=axis, at=at):
                pl.semaphore_signal(ready.at[n], inc=1, device_id={axis: lax.rem(at + 1, 4)}, device_id_type=MESH)

    def origin(d, h):
        back = h - 1
        return lax.rem(z + (Z - back if d == 0 else back), Z)

    def remote(src, dst, kind, recv, d):
        return pltpu.make_async_remote_copy(
            src_ref=src, dst_ref=dst, send_sem=sends.at[kind], recv_sem=recv,
            device_id=towards[d], device_id_type=MESH,
        )

    def half(start, size, d, h):
        return (start, size) if h < 4 else (start + d * (size // 2), size // 2)

    def raw_copy(d, h, n):
        at, size = half(n * BLOCK, BLOCK, d, h)
        there = rawx.at[origin(d, h), pl.ds(at, size)]
        here = train.at[0, pl.ds(at, size)] if h == 1 else there
        recv = raw_r.at[d, h - 1, n] if h < 4 else last.at[RAW]
        return remote(here, there, RAW, recv, d)

    def low_copy(d, h, n):
        ref = lowx.at[x, origin(d, h)]
        recv = last.at[LOW] if ends(LOW, d, h) else low_r.at[d, h - 1]
        return remote(ref, ref, LOW, recv, d)

    def meta_copy(d, h, n):
        ref = meta.at[origin(d, h)]
        recv = last.at[TOP] if ends(TOP, d, h) else meta_r.at[1 - d, h - 1]
        return remote(ref, ref, TOP, recv, d)

    def row_of(m, r, o):
        return m * WHOLE + o * ROWS + r

    def piece_copy(d, h, n, kind=SCALED, part=None):
        m, r = 1 + n * PIECE // ROWS, n * PIECE % ROWS
        at, size = half(row_of(m, r, origin(d, h)), PIECE, d if part is None else part, h)
        ref = out.at[pl.ds(pl.multiple_of(at, size), size)]
        recv = piece_r.at[d, h - 1, n] if h < 4 else last.at[SCALED]
        return remote(ref, ref, kind, recv, d)

    copy_of = (raw_copy, piece_copy, low_copy, meta_copy)

    def goes(kind, h, d):
        return h < 4 or kind in (RAW, SCALED) or d == (1 if kind == LOW else 0)

    def ends(kind, d, h):
        return not goes(kind, h + 1, d) if h < 4 else True

    landed = set()

    def arrived_one(kind, n, h, d):
        if (kind, n, h, d) not in landed and not ends(kind, d, h):
            landed.add((kind, n, h, d))
            copy_of[kind](d, h, n).wait_recv()

    def send(*items):
        for kind, n, h in items:
            for d in (0, 1):
                if h > 1:
                    arrived_one(kind, n, h - 1, d)
                if goes(kind, h, d):
                    copy_of[kind](d, h, n).start()

    def raw(h, *pieces):
        return [(RAW, n, h) for n in pieces]

    def small(h):
        return [(LOW, 0, h), (TOP, 0, h)]

    all_of(train.at[0], load_sem.at[0])
    all_of(lowx.at[x, z], load_sem.at[1])
    raw_copy(0, 1, 0).start()
    raw_copy(0, 1, 1).start()

    @pl.when(z == 0)
    def _():
        pl.semaphore_wait(ready.at[2], 1)

    raw_copy(1, 1, 0).start()
    raw_copy(1, 1, 1).start()
    answer()
    all_of(train.at[pl.ds(1, 2)], load_sem.at[2])
    all_of(low, load_sem.at[3])
    all_of(high, load_sem.at[4])
    all_of(norm_in, load_sem.at[5])
    for m in range(3):
        top = jnp.zeros((8, COLS), jnp.float32)
        for b in range(ROWS // BLOCK):
            rows = pl.ds(b * BLOCK, BLOCK)
            block = fresh_of(low[m, :, rows], high[m], train[m, rows])
            fresh[m, rows] = block
            top = jnp.maximum(top, jnp.max(jnp.abs(block).reshape(BLOCK // 8, 8, COLS), axis=0))
        meta[z, :, pl.ds(m * COLS, COLS)] = jnp.max(top, axis=0, keepdims=True)
    gain = (norm_in[0] + norm_in[1]).astype(jnp.bfloat16)
    lane = lax.broadcasted_iota(jnp.int32, (32, 128), 1)
    entry = lax.broadcasted_iota(jnp.int32, (32, 128), 0)
    place = (lane == entry + 32 * x).astype(jnp.bfloat16)
    meta[z, :, pl.ds(3 * COLS, 128)] = jnp.dot(gain, place, preferred_element_type=jnp.float32)

    send(*small(1), *raw(1, 2, 3), *raw(2, 0))
    send(*small(2), *raw(2, 1, 2))
    send(*small(3), *raw(2, 3), *raw(3, 0, 1))
    send(*small(4), *raw(3, 2, 3), *raw(4, 0))
    all_of(meta.at[pl.ds(0, 2)], last.at[TOP])

    top = jnp.max(meta[:, 0, : 3 * COLS], axis=0, keepdims=True)
    for m, factor in enumerate((factor_q, factor_k, factor_v)):
        of_m = top[:, m * COLS : (m + 1) * COLS]
        factor[...] = of_m[0]
        inverse[m] = 1.0 / of_m

    def scale_own(m, r, size):
        scaled = fresh[m, pl.ds(r, size)] * inverse[m]
        at = pl.multiple_of(row_of(m, r, z), size)
        out[pl.ds(at, size)] = scaled.astype(jnp.bfloat16)

    for j in range(NPIECE):
        scale_own(1 + j * PIECE // ROWS, j * PIECE % ROWS, PIECE)
        if j > 0:
            send((SCALED, j - 1, 1))
    scale_own(0, 0, ROWS)
    send((SCALED, NPIECE - 1, 1))

    def hop(n, buf, at, axis, kind, recv):
        slot, step = ((at, 1), (at, -1), (lax.rem(at + 3, 4), 1))[n]
        return pltpu.make_async_remote_copy(
            src_ref=buf.at[slot], dst_ref=buf.at[slot], send_sem=sends.at[kind],
            recv_sem=recv.at[0 if n == 0 else 1], device_id=beside(axis, at, step, 4), device_id_type=MESH,
        )

    low_x = (lowx, x, "width_1", LOW_X, lx_r)
    gain_x = (norm_x, x, "width_1", NORM_X, nx_r)
    gain_y = (norm_y, y, "width_0", NORM_Y, ny_r)

    def begin(*ring):
        hop(0, *ring).start()
        hop(1, *ring).start()

    def pass_on(*ring):
        hop(0, *ring).wait_recv()
        hop(2, *ring).start()

    def complete(buf, at, axis, kind, recv):
        all_of(buf.at[pl.ds(0, 2)], recv.at[1])

    all_of(lowx.at[0, pl.ds(0, 2)], last.at[LOW])
    norm_x[x] = meta[:, 0, 3 * COLS :]
    for n, (_, at) in enumerate(plane):
        @pl.when(at < 3)
        def _(n=n):
            pl.semaphore_wait(ready.at[n], 2 - lower[n])
    begin(*low_x)
    begin(*gain_x)

    def scale_raw(back):
        o = lax.rem(z + back, Z)
        for b in range(NBLOCK):
            rows = pl.ds(b * BLOCK, BLOCK)
            block = fresh_of(lowx[b, o], high[0], rawx[o, rows])
            at = pl.multiple_of(row_of(0, b * BLOCK, o), BLOCK)
            out[pl.ds(at, BLOCK)] = (block * inverse[0]).astype(jnp.bfloat16)

    send(*raw(4, 1, 2, 3))
    pass_on(*low_x)
    pass_on(*gain_x)
    send((SCALED, 0, 2), (SCALED, 1, 2))
    complete(*low_x)
    complete(*gain_x)
    norm_y[y] = jnp.sum(norm_x[...], axis=0)
    begin(*gain_y)
    scale_raw(1)
    scale_raw(7)
    send((SCALED, 2, 2))
    pass_on(*gain_y)
    scale_raw(2)
    scale_raw(6)
    send((SCALED, 3, 2))
    scale_raw(3)
    scale_raw(5)
    complete(*gain_y)
    for s in range(4):
        for t in range(Z):
            norm_all[pl.ds(t * 4 + s, 1)] = norm_y[s, pl.ds(t, 1)]
    norm[...] = norm_all[...].astype(jnp.bfloat16)
    send((SCALED, 0, 3))
    all_of(rawx.at[0], last.at[RAW])
    scale_raw(4)
    send(*[(SCALED, n, 3) for n in range(1, NPIECE)])

    end = 0
    for d in (0, 1):
        arrived_one(SCALED, end, 3, d)
    piece_copy(1, 4, end).start()
    usual, moved = piece_copy(0, 4, end, MOVED), piece_copy(1, 4, end, MOVED, 0)

    @pl.when(z < Z - 1)
    def _():
        usual.start()

    @pl.when(z == 1)
    def _():
        moved.start()

    send(*[(SCALED, n, 4) for n in range(1, NPIECE)])
    all_of(out.at[pl.ds(0, 2 * ROWS)], last.at[SCALED])

    all_of(out.at[pl.ds(0, 7 * ROWS)], sends.at[RAW])
    all_of(out.at[pl.ds(0, 14 * ROWS - PIECE // 2)], sends.at[SCALED])

    @pl.when(jnp.logical_and(z != 1, z < Z - 1))
    def _():
        usual.wait_send()

    @pl.when(z == 1)
    def _():
        all_of(out.at[pl.ds(0, PIECE)], sends.at[MOVED])

    all_of(lowx.at[0, pl.ds(0, 7)], sends.at[LOW])
    all_of(meta.at[pl.ds(0, 7)], sends.at[TOP])
    all_of(lowx.at[pl.ds(0, 3)], sends.at[LOW_X])
    all_of(norm_x.at[pl.ds(0, 3)], sends.at[NORM_X])
    all_of(norm_y.at[pl.ds(0, 3)], sends.at[NORM_Y])


def write_kernel(weights, fq, fk, fv, gain, sq, sk, sv, oq, ok, ov, og, sem):
    writes = [
        pltpu.make_async_copy(src, dst, sem.at[n])
        for n, (src, dst) in enumerate((
            (weights.at[pl.ds(0, WHOLE)], sq), (weights.at[pl.ds(WHOLE, WHOLE)], sk),
            (weights.at[pl.ds(2 * WHOLE, WHOLE)], sv), (fq, oq), (fk, ok), (fv, ov), (gain, og),
        ))
    ]
    for write in writes:
        write.start()
    for write in writes:
        write.wait()


def per_device(tq, lq, hq, tk, lk, hk, tv, lv, hv, nt, ns):
    hbm = pl.BlockSpec(memory_space=pltpu.HBM)
    vmem = pl.BlockSpec(memory_space=pltpu.VMEM)
    dma = pltpu.SemaphoreType.DMA
    f32, bf16 = jnp.float32, jnp.bfloat16
    args = (tq, lq.T, hq, tk, lk.T, hk, tv, lv.T, hv, nt.reshape(1, 32), ns.reshape(1, 32))
    gathered = pl.pallas_call(
        gather_kernel,
        name="gather_z",
        out_shape=(pltpu.VMEM((3 * WHOLE, COLS), bf16),)
        + (pltpu.VMEM((COLS,), f32),) * 3
        + (pltpu.VMEM((32, 128), bf16),),
        in_specs=[hbm] * 11,
        out_specs=(vmem,) * 5,
        scratch_shapes=[
            pltpu.VMEM((3, ROWS, COLS), bf16),
            pltpu.VMEM((3, 16, ROWS), bf16),
            pltpu.VMEM((3, 16, COLS), bf16),
            pltpu.VMEM((2, 1, 32), f32),
            pltpu.VMEM((3, ROWS, COLS), f32),
            pltpu.VMEM((Z, ROWS, COLS), bf16),
            pltpu.VMEM((4, Z, 16, BLOCK), bf16),
            pltpu.VMEM((Z, 1, META), f32),
            pltpu.VMEM((4, Z, 128), f32),
            pltpu.VMEM((4, Z, 128), f32),
            pltpu.VMEM((32, 128), f32),
            pltpu.VMEM((3, 1, COLS), f32),
            dma((6,)), dma((8,)),
            dma((2, 3, NBLOCK)), dma((2, 3, NPIECE)), dma((2, 3)), dma((2, 3)), dma((4,)),
            dma((2,)), dma((2,)), dma((2,)),
            pltpu.SemaphoreType.REGULAR((3,)),
        ],
        compiler_params=pltpu.CompilerParams(
            collective_id=0, has_side_effects=True, vmem_limit_bytes=32 * 1024 * 1024
        ),
    )(*[pltpu.with_memory_space_constraint(a, pltpu.HBM) for a in args])
    shapes = ((WHOLE, COLS), bf16), ((COLS,), f32)
    sq, sk, sv, fq, fk, fv, gain = pl.pallas_call(
        write_kernel,
        name="write_out",
        out_shape=(jax.ShapeDtypeStruct(*shapes[0]),) * 3
        + (jax.ShapeDtypeStruct(*shapes[1]),) * 3
        + (jax.ShapeDtypeStruct((32, 128), bf16),),
        in_specs=[vmem] * 5,
        out_specs=(hbm,) * 7,
        scratch_shapes=[dma((7,))],
        compiler_params=pltpu.CompilerParams(vmem_limit_bytes=16 * 1024 * 1024),
    )(*gathered)
    return sq, sk, sv, fq, fk, fv, gain.reshape(4096)


def solution(mesh):
    finer = Mesh(
        mesh.devices.reshape(mesh.shape["zero"], 4, 4, mesh.shape["unit"]),
        ("zero", "width_0", "width_1", "unit"),
    )
    matrix, low, high = P(("unit", "zero"), WIDTH), P(("unit", "zero"), None), P("unit", WIDTH)
    return jax.shard_map(
        per_device,
        mesh=finer,
        in_specs=(matrix, low, high) * 3 + (P(UNIT_ZERO_WIDTH), P(UNIT_ZERO_WIDTH)),
        out_specs=(high, high, high, P(UNIT_WIDTH), P(UNIT_WIDTH), P(UNIT_WIDTH), P("unit")),
        check_vma=False,
    )
```

```python
import functools

import jax
import jax.numpy as jnp
from jax import lax
from jax.experimental import pallas as pl
from jax.experimental.pallas import tpu as pltpu
from jax.sharding import Mesh
from jax.sharding import PartitionSpec as P

WIDTH = ("width_0", "width_1")
UNIT_ZERO_WIDTH = ("unit", "zero", "width_0", "width_1")
UNIT_WIDTH = ("unit", "width_0", "width_1")
MESH = pl.DeviceIdType.MESH

mix_rate = 1.0

Z = 8
ROWS = 512
COLS = 256
WHOLE = Z * ROWS
BLOCK = 128
NBLOCK = ROWS // BLOCK
PIECES = ((1, 0, 512), (2, 0, 256), (2, 256, 256))
NPIECE = len(PIECES)
PIECE = 256
META = 1024
RAW, SCALED, LOW, TOP, MOVED = range(5)


def fresh_of(low_t, high, train):
    product = lax.dot_general(
        low_t, high, (((0,), (0,)), ((), ())), preferred_element_type=jnp.float32
    )
    return train.astype(jnp.float32) + mix_rate * product


def gather_kernel(
    tq, lq, hq, tk, lk, hk, tv, lv, hv, nt, ns,
    out, factor_q, factor_k, factor_v, norm,
    train, low, high, norm_in, fresh, rawx, lowx, meta, norm_x, norm_y, norm_all, inverse,
    load_sem, sends, arrivals, meta_r, low_r, low_last, x_r, y_r, ready,
):
    z = lax.axis_index("zero")
    y = lax.axis_index("width_0")
    x = lax.axis_index("width_1")

    lanes = pl.ds(pl.multiple_of(x * BLOCK, BLOCK), BLOCK)
    groups = (
        ((tq, train.at[0]),),
        (
            (tk, train.at[1]), (tv, train.at[2]), (lq, low.at[0]), (lk, low.at[1]), (lv, low.at[2]),
            (hq, high.at[0]), (hk, high.at[1]), (hv, high.at[2]), (lq.at[:, lanes], lowx.at[x, z]),
        ),
        ((nt, norm_in.at[0]), (ns, norm_in.at[1])),
    )
    for n, group in enumerate(groups):
        for src, dst in group:
            pltpu.make_async_copy(src, dst, load_sem.at[n]).start()

    def all_of(ref, sem):
        pltpu.make_async_copy(ref, ref, sem).wait()

    def beside(axis, at, step, size):
        return {axis: lax.rem(at + (step + size), size)}

    towards = (beside("zero", z, 1, Z), beside("zero", z, -1, Z))
    barrier = pltpu.get_barrier_semaphore()
    pl.semaphore_signal(barrier, inc=1, device_id=towards[1], device_id_type=MESH)

    @pl.when(z < Z - 1)
    def _():
        pl.semaphore_signal(barrier, inc=1, device_id=towards[0], device_id_type=MESH)

    plane = (("width_1", x), ("width_0", y))
    for axis, at in plane:
        @pl.when(at < 3)
        def _(axis=axis, at=at):
            pl.semaphore_signal(barrier, inc=1, device_id={axis: lax.rem(at + 1, 4)}, device_id_type=MESH)

        @pl.when(at == 0)
        def _(axis=axis, at=at):
            pl.semaphore_signal(barrier, inc=1, device_id={axis: lax.rem(at + 3, 4)}, device_id_type=MESH)

    lower = [(at + 1) // 2 for _, at in plane]
    pl.semaphore_wait(barrier, 1 + lax.min(z, 1) + lower[0] + lower[1])

    @pl.when(z == Z - 1)
    def _():
        pl.semaphore_signal(ready.at[2], inc=1, device_id=towards[0], device_id_type=MESH)

    def answer():
        for n, (axis, at) in enumerate(plane):
            @pl.when(at > 0)
            def _(n=n, axis=axis, at=at):
                pl.semaphore_signal(ready.at[n], inc=1, device_id={axis: lax.rem(at + 3, 4)}, device_id_type=MESH)

            @pl.when(at == 3)
            def _(n=n, axis=axis, at=at):
                pl.semaphore_signal(ready.at[n], inc=1, device_id={axis: lax.rem(at + 1, 4)}, device_id_type=MESH)

    def origin(d, h):
        back = h - 1
        return lax.rem(z + (Z - back if d == 0 else back), Z)

    def remote(src, dst, kind, recv, d):
        return pltpu.make_async_remote_copy(
            src_ref=src, dst_ref=dst, send_sem=sends.at[kind // MOVED], recv_sem=recv,
            device_id=towards[d], device_id_type=MESH,
        )

    def half(start, size, d, h):
        return (start, size) if h < 4 else (start + d * (size // 2), size // 2)

    def raw_copy(d, h, n):
        at, size = half(n * BLOCK, BLOCK, d, h)
        there = rawx.at[origin(d, h), pl.ds(at, size)]
        here = train.at[0, pl.ds(at, size)] if h == 1 else there
        recv = arrivals.at[d, h - 1, n] if h < 4 else load_sem.at[1]
        return remote(here, there, RAW, recv, d)

    def low_copy(d, h, n):
        ref = lowx.at[x, origin(d, h)]
        recv = low_last if ends(LOW, d, h) else low_r.at[2 * h - 1 - d]
        return remote(ref, ref, LOW, recv, d)

    def meta_copy(d, h, n):
        ref = meta.at[origin(d, h)]
        recv = load_sem.at[2] if ends(TOP, d, h) else meta_r.at[2 * h - 2 + d]
        return remote(ref, ref, TOP, recv, d)

    def row_of(m, r, o):
        return m * WHOLE + o * ROWS + r

    def piece_copy(d, h, n, kind=SCALED, part=None):
        m, r, size = PIECES[n]
        at, size = half(row_of(m, r, origin(d, h)), size, d if part is None else part, h)
        ref = out.at[pl.ds(pl.multiple_of(at, size), size)]
        recv = arrivals.at[d, h - 1, n] if h < 4 else load_sem.at[0]
        return remote(ref, ref, kind, recv, d)

    copy_of = (raw_copy, piece_copy, low_copy, meta_copy)

    def goes(kind, h, d):
        return h < 4 or kind in (RAW, SCALED) or d == (1 if kind == LOW else 0)

    def ends(kind, d, h):
        return not goes(kind, h + 1, d) if h < 4 else True

    landed = set()

    def arrived_one(kind, n, h, d):
        if (kind, n, h, d) not in landed and not ends(kind, d, h):
            landed.add((kind, n, h, d))
            copy_of[kind](d, h, n).wait_recv()

    def send(*items):
        for kind, n, h in items:
            for d in (0, 1):
                if h > 1:
                    arrived_one(kind, n, h - 1, d)
                if goes(kind, h, d):
                    copy_of[kind](d, h, n).start()

    def raw(h, *pieces):
        return [(RAW, n, h) for n in pieces]

    def small(h):
        return [(LOW, 0, h), (TOP, 0, h)]

    all_of(train.at[0], load_sem.at[0])
    raw_copy(0, 1, 0).start()
    raw_copy(0, 1, 1).start()

    @pl.when(z == 0)
    def _():
        pl.semaphore_wait(ready.at[2], 1)

    raw_copy(1, 1, 0).start()
    raw_copy(1, 1, 1).start()
    answer()
    all_of(out.at[pl.ds(0, 2 * ROWS + 152)], load_sem.at[1])
    all_of(norm_in, load_sem.at[2])
    for m in range(3):
        top = jnp.zeros((8, COLS), jnp.float32)
        for b in range(ROWS // BLOCK):
            rows = pl.ds(b * BLOCK, BLOCK)
            block = fresh_of(low[m, :, rows], high[m], train[m, rows])
            fresh[m, rows] = block
            top = jnp.maximum(top, jnp.max(jnp.abs(block).reshape(BLOCK // 8, 8, COLS), axis=0))
        meta[z, :, pl.ds(m * COLS, COLS)] = jnp.max(top, axis=0, keepdims=True)
    gain = (norm_in[0] + norm_in[1]).astype(jnp.bfloat16)
    lane = lax.broadcasted_iota(jnp.int32, (32, 128), 1)
    entry = lax.broadcasted_iota(jnp.int32, (32, 128), 0)
    place = (lane == entry + 32 * x).astype(jnp.bfloat16)
    meta[z, :, pl.ds(3 * COLS, 128)] = jnp.dot(gain, place, preferred_element_type=jnp.float32)

    send(*small(1), *raw(1, 2, 3), *raw(2, 0))
    send(*small(2), *raw(2, 1, 2))
    send(*small(3), *raw(2, 3), *raw(3, 0, 1))
    send(*small(4), *raw(3, 2, 3), *raw(4, 0))
    all_of(meta.at[pl.ds(0, 2)], load_sem.at[2])

    top = jnp.max(meta[:, 0, : 3 * COLS], axis=0, keepdims=True)
    for m, factor in enumerate((factor_q, factor_k, factor_v)):
        of_m = top[:, m * COLS : (m + 1) * COLS]
        factor[...] = of_m[0]
        inverse[m] = 1.0 / of_m

    def scale_own(m, r, size):
        scaled = fresh[m, pl.ds(r, size)] * inverse[m]
        at = pl.multiple_of(row_of(m, r, z), size)
        out[pl.ds(at, size)] = scaled.astype(jnp.bfloat16)

    for j in range(NPIECE):
        scale_own(*PIECES[j])
        if j > 0:
            send((SCALED, j - 1, 1))
    scale_own(0, 0, ROWS)
    send((SCALED, NPIECE - 1, 1))

    def hop(n, buf, at, axis, recv):
        slot, step = ((at, 1), (at, -1), (lax.rem(at + 3, 4), 1))[n]
        return pltpu.make_async_remote_copy(
            src_ref=buf.at[slot], dst_ref=buf.at[slot], send_sem=sends.at[0],
            recv_sem=recv.at[0 if n == 0 else 1], device_id=beside(axis, at, step, 4), device_id_type=MESH,
        )

    low_x = (lowx, x, "width_1", x_r)
    gain_x = (norm_x, x, "width_1", x_r)
    gain_y = (norm_y, y, "width_0", y_r)

    def begin(*ring):
        hop(0, *ring).start()
        hop(1, *ring).start()

    def sizes(n, *rings):
        return out.at[pl.ds(0, n * sum(8 if ring[0] is not lowx else 64 for ring in rings))]

    def pass_on(*rings):
        all_of(sizes(1, *rings), rings[0][-1].at[0])
        for ring in rings:
            hop(2, *ring).start()

    def complete(*rings):
        all_of(sizes(2, *rings), rings[0][-1].at[1])

    all_of(lowx.at[0, pl.ds(0, 2)], low_last)
    norm_x[x] = meta[:, 0, 3 * COLS : 3 * COLS + 128]
    for n, (_, at) in enumerate(plane):
        @pl.when(at < 3)
        def _(n=n):
            pl.semaphore_wait(ready.at[n], 2 - lower[n])
    begin(*low_x)
    begin(*gain_x)

    def scale_raw(back):
        o = lax.rem(z + back, Z)
        for b in range(NBLOCK):
            rows = pl.ds(b * BLOCK, BLOCK)
            block = fresh_of(lowx[b, o], high[0], rawx[o, rows])
            at = pl.multiple_of(row_of(0, b * BLOCK, o), BLOCK)
            out[pl.ds(at, BLOCK)] = (block * inverse[0]).astype(jnp.bfloat16)

    send(*raw(4, 1, 2, 3))
    pass_on(low_x, gain_x)
    send((SCALED, 0, 2), (SCALED, 1, 2))
    complete(low_x, gain_x)
    norm_y[y] = jnp.sum(norm_x[...], axis=0)
    begin(*gain_y)
    scale_raw(1)
    scale_raw(7)
    pass_on(gain_y)
    scale_raw(2)
    scale_raw(6)
    send((SCALED, 2, 2))
    scale_raw(3)
    scale_raw(5)
    complete(gain_y)
    for s in range(4):
        for t in range(Z):
            norm_all[pl.ds(t * 4 + s, 1)] = norm_y[s, pl.ds(t, 1)]
    norm[...] = norm_all[...].astype(jnp.bfloat16)
    send((SCALED, 0, 3))
    all_of(rawx.at[0], load_sem.at[1])
    scale_raw(4)
    send(*[(SCALED, n, 3) for n in range(1, NPIECE)])

    send((SCALED, 0, 4))
    end = 1
    for d in (0, 1):
        arrived_one(SCALED, end, 3, d)
    piece_copy(1, 4, end).start()
    usual, moved = piece_copy(0, 4, end, MOVED), piece_copy(1, 4, end, MOVED, 0)

    @pl.when(z < Z - 1)
    def _():
        usual.start()

    @pl.when(z == 1)
    def _():
        moved.start()

    send((SCALED, 2, 4))
    all_of(out.at[pl.ds(0, 2 * ROWS)], load_sem.at[0])

    all_of(out.at[pl.ds(0, 21 * ROWS - PIECE // 2 + 14 * 8 + 3 * (64 + 8 + 8))], sends.at[0])

    @pl.when(jnp.logical_and(z != 1, z < Z - 1))
    def _():
        usual.wait_send()

    @pl.when(z == 1)
    def _():
        all_of(out.at[pl.ds(0, PIECE)], sends.at[1])


def write_kernel(weights, fq, fk, fv, gain, sq, sk, sv, oq, ok, ov, og, sem):
    writes = [
        pltpu.make_async_copy(src, dst, sem.at[n])
        for n, (src, dst) in enumerate((
            (weights.at[pl.ds(0, WHOLE)], sq), (weights.at[pl.ds(WHOLE, WHOLE)], sk),
            (weights.at[pl.ds(2 * WHOLE, WHOLE)], sv), (fq, oq), (fk, ok), (fv, ov), (gain, og),
        ))
    ]
    for write in writes:
        write.start()
    for write in writes:
        write.wait()


def per_device(tq, lq, hq, tk, lk, hk, tv, lv, hv, nt, ns):
    hbm = pl.BlockSpec(memory_space=pltpu.HBM)
    vmem = pl.BlockSpec(memory_space=pltpu.VMEM)
    dma = pltpu.SemaphoreType.DMA
    f32, bf16 = jnp.float32, jnp.bfloat16
    args = (tq, lq.T, hq, tk, lk.T, hk, tv, lv.T, hv, nt.reshape(1, 32), ns.reshape(1, 32))
    gathered = pl.pallas_call(
        gather_kernel,
        name="gather_z",
        out_shape=(pltpu.VMEM((3 * WHOLE, COLS), bf16),)
        + (pltpu.VMEM((COLS,), f32),) * 3
        + (pltpu.VMEM((32, 128), bf16),),
        in_specs=[hbm] * 11,
        out_specs=(vmem,) * 5,
        scratch_shapes=[
            pltpu.VMEM((3, ROWS, COLS), bf16),
            pltpu.VMEM((3, 16, ROWS), bf16),
            pltpu.VMEM((3, 16, COLS), bf16),
            pltpu.VMEM((2, 1, 32), f32),
            pltpu.VMEM((3, ROWS, COLS), f32),
            pltpu.VMEM((Z, ROWS, COLS), bf16),
            pltpu.VMEM((4, Z, 16, BLOCK), bf16),
            pltpu.VMEM((Z, 1, META), f32),
            pltpu.VMEM((4, Z, 128), f32),
            pltpu.VMEM((4, Z, 128), f32),
            pltpu.VMEM((32, 128), f32),
            pltpu.VMEM((3, 1, COLS), f32),
            dma((3,)), dma((2,)),
            dma((2, 3, NBLOCK)), dma((5,)), dma((5,)), dma,
            dma((2,)), dma((2,)),
            pltpu.SemaphoreType.REGULAR((3,)),
        ],
        compiler_params=pltpu.CompilerParams(
            collective_id=0, has_side_effects=True, vmem_limit_bytes=32 * 1024 * 1024
        ),
    )(*[pltpu.with_memory_space_constraint(a, pltpu.HBM) for a in args])
    shapes = ((WHOLE, COLS), bf16), ((COLS,), f32)
    sq, sk, sv, fq, fk, fv, gain = pl.pallas_call(
        write_kernel,
        name="write_out",
        out_shape=(jax.ShapeDtypeStruct(*shapes[0]),) * 3
        + (jax.ShapeDtypeStruct(*shapes[1]),) * 3
        + (jax.ShapeDtypeStruct((32, 128), bf16),),
        in_specs=[vmem] * 5,
        out_specs=(hbm,) * 7,
        scratch_shapes=[dma((7,))],
        compiler_params=pltpu.CompilerParams(vmem_limit_bytes=16 * 1024 * 1024),
    )(*gathered)
    return sq, sk, sv, fq, fk, fv, gain.reshape(4096)


def solution(mesh):
    finer = Mesh(
        mesh.devices.reshape(mesh.shape["zero"], 4, 4, mesh.shape["unit"]),
        ("zero", "width_0", "width_1", "unit"),
    )
    matrix, low, high = P(("unit", "zero"), WIDTH), P(("unit", "zero"), None), P("unit", WIDTH)
    return jax.shard_map(
        per_device,
        mesh=finer,
        in_specs=(matrix, low, high) * 3 + (P(UNIT_ZERO_WIDTH), P(UNIT_ZERO_WIDTH)),
        out_specs=(high, high, high, P(UNIT_WIDTH), P(UNIT_WIDTH), P(UNIT_WIDTH), P("unit")),
        check_vma=False,
    )
```

```python
import functools

import jax
import jax.numpy as jnp
from jax import lax
from jax.experimental import pallas as pl
from jax.experimental.pallas import tpu as pltpu
from jax.sharding import Mesh
from jax.sharding import PartitionSpec as P

WIDTH = ("width_0", "width_1")
UNIT_ZERO_WIDTH = ("unit", "zero", "width_0", "width_1")
UNIT_WIDTH = ("unit", "width_0", "width_1")
MESH = pl.DeviceIdType.MESH

mix_rate = 1.0

Z = 8
ROWS = 512
COLS = 256
WHOLE = Z * ROWS
BLOCK = 128
NBLOCK = ROWS // BLOCK
PIECES = ((1, 0, 512), (2, 0, 256), (2, 256, 256))
NPIECE = len(PIECES)
PIECE = 256
META = 1024
RAW, SCALED, LOW, TOP, MOVED = range(5)


def fresh_of(low_t, high, train):
    product = lax.dot_general(
        low_t, high, (((0,), (0,)), ((), ())), preferred_element_type=jnp.float32
    )
    return train.astype(jnp.float32) + mix_rate * product


def gather_kernel(
    tq, lq, hq, tk, lk, hk, tv, lv, hv, nt, ns,
    out, factor_q, factor_k, factor_v, norm,
    train, low, high, norm_in, fresh, rawx, lowx, meta, norm_x, norm_y, norm_all, inverse,
    load_sem, sends, arrivals, meta_r, low_r, low_last, x_r, y_r, ready,
):
    z = lax.axis_index("zero")
    y = lax.axis_index("width_0")
    x = lax.axis_index("width_1")

    lanes = pl.ds(pl.multiple_of(x * BLOCK, BLOCK), BLOCK)
    groups = (
        ((tq, train.at[0]),),
        (
            (tk, train.at[1]), (tv, train.at[2]), (lq, low.at[0]), (lk, low.at[1]), (lv, low.at[2]),
            (hq, high.at[0]), (hk, high.at[1]), (hv, high.at[2]), (lq.at[:, lanes], lowx.at[x, z]),
        ),
        ((nt, norm_in.at[0]), (ns, norm_in.at[1])),
    )
    for n, group in enumerate(groups):
        for src, dst in group:
            pltpu.make_async_copy(src, dst, load_sem.at[n]).start()

    def all_of(ref, sem):
        pltpu.make_async_copy(ref, ref, sem).wait()

    def beside(axis, at, step, size):
        return {axis: lax.rem(at + (step + size), size)}

    towards = (beside("zero", z, 1, Z), beside("zero", z, -1, Z))
    barrier = pltpu.get_barrier_semaphore()
    pl.semaphore_signal(barrier, inc=1, device_id=towards[1], device_id_type=MESH)

    @pl.when(z < Z - 1)
    def _():
        pl.semaphore_signal(barrier, inc=1, device_id=towards[0], device_id_type=MESH)

    plane = (("width_1", x), ("width_0", y))
    for axis, at in plane:
        @pl.when(at < 3)
        def _(axis=axis, at=at):
            pl.semaphore_signal(barrier, inc=1, device_id={axis: lax.rem(at + 1, 4)}, device_id_type=MESH)

        @pl.when(at == 0)
        def _(axis=axis, at=at):
            pl.semaphore_signal(barrier, inc=1, device_id={axis: lax.rem(at + 3, 4)}, device_id_type=MESH)

    lower = [(at + 1) // 2 for _, at in plane]
    pl.semaphore_wait(barrier, 1 + lax.min(z, 1) + lower[0] + lower[1])

    @pl.when(z == Z - 1)
    def _():
        pl.semaphore_signal(ready.at[2], inc=1, device_id=towards[0], device_id_type=MESH)

    def answer():
        for n, (axis, at) in enumerate(plane):
            @pl.when(at > 0)
            def _(n=n, axis=axis, at=at):
                pl.semaphore_signal(ready.at[n], inc=1, device_id={axis: lax.rem(at + 3, 4)}, device_id_type=MESH)

            @pl.when(at == 3)
            def _(n=n, axis=axis, at=at):
                pl.semaphore_signal(ready.at[n], inc=1, device_id={axis: lax.rem(at + 1, 4)}, device_id_type=MESH)

    def origin(d, h):
        back = h - 1
        return lax.rem(z + (Z - back if d == 0 else back), Z)

    def remote(src, dst, kind, recv, d):
        return pltpu.make_async_remote_copy(
            src_ref=src, dst_ref=dst, send_sem=sends.at[kind // MOVED], recv_sem=recv,
            device_id=towards[d], device_id_type=MESH,
        )

    def half(start, size, d, h):
        return (start, size) if h < 4 else (start + d * (size // 2), size // 2)

    def raw_copy(d, h, n):
        at, size = half(n * BLOCK, BLOCK, d, h)
        there = rawx.at[origin(d, h), pl.ds(at, size)]
        here = train.at[0, pl.ds(at, size)] if h == 1 else there
        recv = arrivals.at[d, h - 1, n] if h < 4 else load_sem.at[1]
        return remote(here, there, RAW, recv, d)

    def low_copy(d, h, n):
        ref = lowx.at[x, origin(d, h)]
        recv = low_last if ends(LOW, d, h) else low_r.at[2 * h - 1 - d]
        return remote(ref, ref, LOW, recv, d)

    def meta_copy(d, h, n):
        ref = meta.at[origin(d, h)]
        recv = load_sem.at[2] if ends(TOP, d, h) else meta_r.at[2 * h - 2 + d]
        return remote(ref, ref, TOP, recv, d)

    def row_of(m, r, o):
        return m * WHOLE + o * ROWS + r

    def piece_copy(d, h, n, kind=SCALED, part=None):
        m, r, size = PIECES[n]
        at, size = half(row_of(m, r, origin(d, h)), size, d if part is None else part, h)
        ref = out.at[pl.ds(pl.multiple_of(at, size), size)]
        recv = arrivals.at[d, h - 1, n] if h < 4 else load_sem.at[0]
        return remote(ref, ref, kind, recv, d)

    copy_of = (raw_copy, piece_copy, low_copy, meta_copy)

    def goes(kind, h, d):
        return h < 4 or kind in (RAW, SCALED) or d == (1 if kind == LOW else 0)

    def ends(kind, d, h):
        return not goes(kind, h + 1, d) if h < 4 else True

    landed = set()

    def arrived_one(kind, n, h, d):
        if (kind, n, h, d) not in landed and not ends(kind, d, h):
            landed.add((kind, n, h, d))
            copy_of[kind](d, h, n).wait_recv()

    def send(*items):
        for kind, n, h in items:
            for d in (0, 1):
                if h > 1:
                    arrived_one(kind, n, h - 1, d)
                if goes(kind, h, d):
                    copy_of[kind](d, h, n).start()

    def raw(h, *pieces):
        return [(RAW, n, h) for n in pieces]

    def small(h):
        return [(LOW, 0, h), (TOP, 0, h)]

    all_of(train.at[0], load_sem.at[0])
    def first():
        raw_copy(0, 1, 0).start()
        raw_copy(0, 1, 1).start()

        @pl.when(z == 0)
        def _():
            pl.semaphore_wait(ready.at[2], 1)

        raw_copy(1, 1, 0).start()
        raw_copy(1, 1, 1).start()

    unit = lax.axis_index("unit")

    @pl.when(unit == 0)
    def _():
        first()

    answer()
    all_of(out.at[pl.ds(0, 2 * ROWS + 152)], load_sem.at[1])
    all_of(norm_in, load_sem.at[2])
    for m in range(3):
        top = jnp.zeros((8, COLS), jnp.float32)
        for b in range(ROWS // BLOCK):
            rows = pl.ds(b * BLOCK, BLOCK)
            block = fresh_of(low[m, :, rows], high[m], train[m, rows])
            fresh[m, rows] = block
            top = jnp.maximum(top, jnp.max(jnp.abs(block).reshape(BLOCK // 8, 8, COLS), axis=0))
        meta[z, :, pl.ds(m * COLS, COLS)] = jnp.max(top, axis=0, keepdims=True)
    gain = (norm_in[0] + norm_in[1]).astype(jnp.bfloat16)
    lane = lax.broadcasted_iota(jnp.int32, (32, 128), 1)
    entry = lax.broadcasted_iota(jnp.int32, (32, 128), 0)
    place = (lane == entry + 32 * x).astype(jnp.bfloat16)
    meta[z, :, pl.ds(3 * COLS, 128)] = jnp.dot(gain, place, preferred_element_type=jnp.float32)

    @pl.when(unit == 1)
    def _():
        first()

    send(*small(1), *raw(1, 2, 3), *raw(2, 0))
    send(*small(2), *raw(2, 1, 2))
    send(*small(3), *raw(2, 3), *raw(3, 0, 1))
    send(*small(4), *raw(3, 2, 3), *raw(4, 0))
    all_of(meta.at[pl.ds(0, 2)], load_sem.at[2])

    top = jnp.max(meta[:, 0, : 3 * COLS], axis=0, keepdims=True)
    for m, factor in enumerate((factor_q, factor_k, factor_v)):
        of_m = top[:, m * COLS : (m + 1) * COLS]
        factor[...] = of_m[0]
        inverse[m] = 1.0 / of_m

    def scale_own(m, r, size):
        scaled = fresh[m, pl.ds(r, size)] * inverse[m]
        at = pl.multiple_of(row_of(m, r, z), size)
        out[pl.ds(at, size)] = scaled.astype(jnp.bfloat16)

    for j in range(NPIECE):
        scale_own(*PIECES[j])
        if j > 0:
            send((SCALED, j - 1, 1))
    scale_own(0, 0, ROWS)
    send((SCALED, NPIECE - 1, 1))

    def hop(n, buf, at, axis, recv):
        slot, step = ((at, 1), (at, -1), (lax.rem(at + 3, 4), 1))[n]
        return pltpu.make_async_remote_copy(
            src_ref=buf.at[slot], dst_ref=buf.at[slot], send_sem=sends.at[0],
            recv_sem=recv.at[0 if n == 0 else 1], device_id=beside(axis, at, step, 4), device_id_type=MESH,
        )

    low_x = (lowx, x, "width_1", x_r)
    gain_x = (norm_x, x, "width_1", x_r)
    gain_y = (norm_y, y, "width_0", y_r)

    def begin(*ring):
        hop(0, *ring).start()
        hop(1, *ring).start()

    def sizes(n, *rings):
        return out.at[pl.ds(0, n * sum(8 if ring[0] is not lowx else 64 for ring in rings))]

    def pass_on(*rings):
        all_of(sizes(1, *rings), rings[0][-1].at[0])
        for ring in rings:
            hop(2, *ring).start()

    def complete(*rings):
        all_of(sizes(2, *rings), rings[0][-1].at[1])

    all_of(lowx.at[0, pl.ds(0, 2)], low_last)
    norm_x[x] = meta[:, 0, 3 * COLS : 3 * COLS + 128]
    for n, (_, at) in enumerate(plane):
        @pl.when(at < 3)
        def _(n=n):
            pl.semaphore_wait(ready.at[n], 2 - lower[n])
    begin(*low_x)
    begin(*gain_x)

    def scale_raw(back):
        o = lax.rem(z + back, Z)
        for b in range(NBLOCK):
            rows = pl.ds(b * BLOCK, BLOCK)
            block = fresh_of(lowx[b, o], high[0], rawx[o, rows])
            at = pl.multiple_of(row_of(0, b * BLOCK, o), BLOCK)
            out[pl.ds(at, BLOCK)] = (block * inverse[0]).astype(jnp.bfloat16)

    send(*raw(4, 1, 2, 3))
    pass_on(low_x, gain_x)
    send((SCALED, 0, 2), (SCALED, 1, 2))
    complete(low_x, gain_x)
    norm_y[y] = jnp.sum(norm_x[...], axis=0)
    begin(*gain_y)
    scale_raw(1)
    scale_raw(7)
    pass_on(gain_y)
    scale_raw(2)
    scale_raw(6)
    send((SCALED, 2, 2))
    scale_raw(3)
    scale_raw(5)
    complete(gain_y)
    for s in range(4):
        for t in range(Z):
            norm_all[pl.ds(t * 4 + s, 1)] = norm_y[s, pl.ds(t, 1)]
    norm[...] = norm_all[...].astype(jnp.bfloat16)
    send((SCALED, 0, 3))
    all_of(rawx.at[0], load_sem.at[1])
    scale_raw(4)
    send(*[(SCALED, n, 3) for n in range(1, NPIECE)])

    send((SCALED, 0, 4))
    end = 1
    for d in (0, 1):
        arrived_one(SCALED, end, 3, d)
    piece_copy(1, 4, end).start()
    usual, moved = piece_copy(0, 4, end, MOVED), piece_copy(1, 4, end, MOVED, 0)

    @pl.when(z < Z - 1)
    def _():
        usual.start()

    @pl.when(z == 1)
    def _():
        moved.start()

    send((SCALED, 2, 4))
    all_of(out.at[pl.ds(0, 2 * ROWS)], load_sem.at[0])

    all_of(out.at[pl.ds(0, 21 * ROWS - PIECE // 2 + 14 * 8 + 3 * (64 + 8 + 8))], sends.at[0])

    @pl.when(jnp.logical_and(z != 1, z < Z - 1))
    def _():
        usual.wait_send()

    @pl.when(z == 1)
    def _():
        all_of(out.at[pl.ds(0, PIECE)], sends.at[1])


def write_kernel(weights, fq, fk, fv, gain, sq, sk, sv, oq, ok, ov, og, sem):
    writes = [
        pltpu.make_async_copy(src, dst, sem.at[n])
        for n, (src, dst) in enumerate((
            (weights.at[pl.ds(0, WHOLE)], sq), (weights.at[pl.ds(WHOLE, WHOLE)], sk),
            (weights.at[pl.ds(2 * WHOLE, WHOLE)], sv), (fq, oq), (fk, ok), (fv, ov), (gain, og),
        ))
    ]
    for write in writes:
        write.start()
    for write in writes:
        write.wait()


def per_device(tq, lq, hq, tk, lk, hk, tv, lv, hv, nt, ns):
    hbm = pl.BlockSpec(memory_space=pltpu.HBM)
    vmem = pl.BlockSpec(memory_space=pltpu.VMEM)
    dma = pltpu.SemaphoreType.DMA
    f32, bf16 = jnp.float32, jnp.bfloat16
    args = (tq, lq.T, hq, tk, lk.T, hk, tv, lv.T, hv, nt.reshape(1, 32), ns.reshape(1, 32))
    gathered = pl.pallas_call(
        gather_kernel,
        name="gather_z",
        out_shape=(pltpu.VMEM((3 * WHOLE, COLS), bf16),)
        + (pltpu.VMEM((COLS,), f32),) * 3
        + (pltpu.VMEM((32, 128), bf16),),
        in_specs=[hbm] * 11,
        out_specs=(vmem,) * 5,
        scratch_shapes=[
            pltpu.VMEM((3, ROWS, COLS), bf16),
            pltpu.VMEM((3, 16, ROWS), bf16),
            pltpu.VMEM((3, 16, COLS), bf16),
            pltpu.VMEM((2, 1, 32), f32),
            pltpu.VMEM((3, ROWS, COLS), f32),
            pltpu.VMEM((Z, ROWS, COLS), bf16),
            pltpu.VMEM((4, Z, 16, BLOCK), bf16),
            pltpu.VMEM((Z, 1, META), f32),
            pltpu.VMEM((4, Z, 128), f32),
            pltpu.VMEM((4, Z, 128), f32),
            pltpu.VMEM((32, 128), f32),
            pltpu.VMEM((3, 1, COLS), f32),
            dma((3,)), dma((2,)),
            dma((2, 3, NBLOCK)), dma((5,)), dma((5,)), dma,
            dma((2,)), dma((2,)),
            pltpu.SemaphoreType.REGULAR((3,)),
        ],
        compiler_params=pltpu.CompilerParams(
            collective_id=0, has_side_effects=True, vmem_limit_bytes=32 * 1024 * 1024
        ),
    )(*[pltpu.with_memory_space_constraint(a, pltpu.HBM) for a in args])
    shapes = ((WHOLE, COLS), bf16), ((COLS,), f32)
    sq, sk, sv, fq, fk, fv, gain = pl.pallas_call(
        write_kernel,
        name="write_out",
        out_shape=(jax.ShapeDtypeStruct(*shapes[0]),) * 3
        + (jax.ShapeDtypeStruct(*shapes[1]),) * 3
        + (jax.ShapeDtypeStruct((32, 128), bf16),),
        in_specs=[vmem] * 5,
        out_specs=(hbm,) * 7,
        scratch_shapes=[dma((7,))],
        compiler_params=pltpu.CompilerParams(vmem_limit_bytes=16 * 1024 * 1024),
    )(*gathered)
    return sq, sk, sv, fq, fk, fv, gain.reshape(4096)


def solution(mesh):
    finer = Mesh(
        mesh.devices.reshape(mesh.shape["zero"], 4, 4, mesh.shape["unit"]),
        ("zero", "width_0", "width_1", "unit"),
    )
    matrix, low, high = P(("unit", "zero"), WIDTH), P(("unit", "zero"), None), P("unit", WIDTH)
    return jax.shard_map(
        per_device,
        mesh=finer,
        in_specs=(matrix, low, high) * 3 + (P(UNIT_ZERO_WIDTH), P(UNIT_ZERO_WIDTH)),
        out_specs=(high, high, high, P(UNIT_WIDTH), P(UNIT_WIDTH), P(UNIT_WIDTH), P("unit")),
        check_vma=False,
    )
```

```python
import functools

import jax
import jax.numpy as jnp
from jax import lax
from jax.experimental import pallas as pl
from jax.experimental.pallas import tpu as pltpu
from jax.sharding import Mesh
from jax.sharding import PartitionSpec as P

WIDTH = ("width_0", "width_1")
UNIT_ZERO_WIDTH = ("unit", "zero", "width_0", "width_1")
UNIT_WIDTH = ("unit", "width_0", "width_1")
MESH = pl.DeviceIdType.MESH

mix_rate = 1.0

Z = 8
ROWS = 512
COLS = 256
WHOLE = Z * ROWS
BLOCK = 128
NBLOCK = ROWS // BLOCK
PIECES = ((1, 0, 512), (2, 0, 320), (2, 320, 192))
NPIECE = len(PIECES)
PIECE = 320
META = 1024
RAW, SCALED, LOW, TOP, MOVED = range(5)


def fresh_of(low_t, high, train):
    product = lax.dot_general(
        low_t, high, (((0,), (0,)), ((), ())), preferred_element_type=jnp.float32
    )
    return train.astype(jnp.float32) + mix_rate * product


def gather_kernel(
    tq, lq, hq, tk, lk, hk, tv, lv, hv, nt, ns,
    out, factor_q, factor_k, factor_v, norm,
    train, low, high, norm_in, fresh, rawx, lowx, meta, norm_x, norm_y, norm_all, inverse,
    load_sem, sends, arrivals, meta_r, low_r, low_last, x_r, y_r, ready,
):
    z = lax.axis_index("zero")
    y = lax.axis_index("width_0")
    x = lax.axis_index("width_1")

    lanes = pl.ds(pl.multiple_of(x * BLOCK, BLOCK), BLOCK)
    groups = (
        ((tq, train.at[0]),),
        (
            (tk, train.at[1]), (tv, train.at[2]), (lq, low.at[0]), (lk, low.at[1]), (lv, low.at[2]),
            (hq, high.at[0]), (hk, high.at[1]), (hv, high.at[2]), (lq.at[:, lanes], lowx.at[x, z]),
        ),
        ((nt, norm_in.at[0]), (ns, norm_in.at[1])),
    )
    for n, group in enumerate(groups):
        for src, dst in group:
            pltpu.make_async_copy(src, dst, load_sem.at[n]).start()

    def all_of(ref, sem):
        pltpu.make_async_copy(ref, ref, sem).wait()

    def beside(axis, at, step, size):
        return {axis: lax.rem(at + (step + size), size)}

    towards = (beside("zero", z, 1, Z), beside("zero", z, -1, Z))
    barrier = pltpu.get_barrier_semaphore()
    pl.semaphore_signal(barrier, inc=1, device_id=towards[1], device_id_type=MESH)

    @pl.when(z < Z - 1)
    def _():
        pl.semaphore_signal(barrier, inc=1, device_id=towards[0], device_id_type=MESH)

    plane = (("width_1", x), ("width_0", y))
    for axis, at in plane:
        @pl.when(at < 3)
        def _(axis=axis, at=at):
            pl.semaphore_signal(barrier, inc=1, device_id={axis: lax.rem(at + 1, 4)}, device_id_type=MESH)

        @pl.when(at == 0)
        def _(axis=axis, at=at):
            pl.semaphore_signal(barrier, inc=1, device_id={axis: lax.rem(at + 3, 4)}, device_id_type=MESH)

    lower = [(at + 1) // 2 for _, at in plane]
    pl.semaphore_wait(barrier, 1 + lax.min(z, 1) + lower[0] + lower[1])

    @pl.when(z == Z - 1)
    def _():
        pl.semaphore_signal(ready.at[2], inc=1, device_id=towards[0], device_id_type=MESH)

    def answer():
        for n, (axis, at) in enumerate(plane):
            @pl.when(at > 0)
            def _(n=n, axis=axis, at=at):
                pl.semaphore_signal(ready.at[n], inc=1, device_id={axis: lax.rem(at + 3, 4)}, device_id_type=MESH)

            @pl.when(at == 3)
            def _(n=n, axis=axis, at=at):
                pl.semaphore_signal(ready.at[n], inc=1, device_id={axis: lax.rem(at + 1, 4)}, device_id_type=MESH)

    def origin(d, h):
        back = h - 1
        return lax.rem(z + (Z - back if d == 0 else back), Z)

    def remote(src, dst, kind, recv, d):
        return pltpu.make_async_remote_copy(
            src_ref=src, dst_ref=dst, send_sem=sends.at[kind // MOVED], recv_sem=recv,
            device_id=towards[d], device_id_type=MESH,
        )

    def half(start, size, d, h):
        return (start, size) if h < 4 else (start + d * (size // 2), size // 2)

    def raw_copy(d, h, n):
        at, size = half(n * BLOCK, BLOCK, d, h)
        there = rawx.at[origin(d, h), pl.ds(at, size)]
        here = train.at[0, pl.ds(at, size)] if h == 1 else there
        recv = arrivals.at[d, h - 1, n] if h < 4 else load_sem.at[1]
        return remote(here, there, RAW, recv, d)

    def low_copy(d, h, n):
        ref = lowx.at[x, origin(d, h)]
        recv = low_last if ends(LOW, d, h) else low_r.at[2 * h - 1 - d]
        return remote(ref, ref, LOW, recv, d)

    def meta_copy(d, h, n):
        ref = meta.at[origin(d, h)]
        recv = load_sem.at[2] if ends(TOP, d, h) else meta_r.at[2 * h - 2 + d]
        return remote(ref, ref, TOP, recv, d)

    def row_of(m, r, o):
        return m * WHOLE + o * ROWS + r

    def piece_copy(d, h, n, kind=SCALED, part=None):
        m, r, size = PIECES[n]
        at, size = half(row_of(m, r, origin(d, h)), size, d if part is None else part, h)
        ref = out.at[pl.ds(pl.multiple_of(at, 32), size)]
        recv = arrivals.at[d, h - 1, n] if h < 4 else load_sem.at[0]
        return remote(ref, ref, kind, recv, d)

    copy_of = (raw_copy, piece_copy, low_copy, meta_copy)

    def goes(kind, h, d):
        return h < 4 or kind in (RAW, SCALED) or d == (1 if kind == LOW else 0)

    def ends(kind, d, h):
        return not goes(kind, h + 1, d) if h < 4 else True

    landed = set()

    def arrived_one(kind, n, h, d):
        if (kind, n, h, d) not in landed and not ends(kind, d, h):
            landed.add((kind, n, h, d))
            copy_of[kind](d, h, n).wait_recv()

    def send(*items):
        for kind, n, h in items:
            for d in (0, 1):
                if h > 1:
                    arrived_one(kind, n, h - 1, d)
                if goes(kind, h, d):
                    copy_of[kind](d, h, n).start()

    def raw(h, *pieces):
        return [(RAW, n, h) for n in pieces]

    def small(h):
        return [(LOW, 0, h), (TOP, 0, h)]

    all_of(train.at[0], load_sem.at[0])
    raw_copy(0, 1, 0).start()
    raw_copy(0, 1, 1).start()

    @pl.when(z == 0)
    def _():
        pl.semaphore_wait(ready.at[2], 1)

    raw_copy(1, 1, 0).start()
    raw_copy(1, 1, 1).start()
    answer()
    all_of(out.at[pl.ds(0, 2 * ROWS + 152)], load_sem.at[1])
    all_of(norm_in, load_sem.at[2])
    for m in range(3):
        top = jnp.zeros((8, COLS), jnp.float32)
        for b in range(ROWS // BLOCK):
            rows = pl.ds(b * BLOCK, BLOCK)
            block = fresh_of(low[m, :, rows], high[m], train[m, rows])
            fresh[m, rows] = block
            top = jnp.maximum(top, jnp.max(jnp.abs(block).reshape(BLOCK // 8, 8, COLS), axis=0))
        meta[z, :, pl.ds(m * COLS, COLS)] = jnp.max(top, axis=0, keepdims=True)
    gain = (norm_in[0] + norm_in[1]).astype(jnp.bfloat16)
    lane = lax.broadcasted_iota(jnp.int32, (32, 128), 1)
    entry = lax.broadcasted_iota(jnp.int32, (32, 128), 0)
    place = (lane == entry + 32 * x).astype(jnp.bfloat16)
    meta[z, :, pl.ds(3 * COLS, 128)] = jnp.dot(gain, place, preferred_element_type=jnp.float32)

    send(*small(1), *raw(1, 2, 3), *raw(2, 0))
    send(*small(2), *raw(2, 1, 2))
    send(*small(3), *raw(2, 3), *raw(3, 0, 1))
    send(*small(4), *raw(3, 2, 3), *raw(4, 0))
    all_of(meta.at[pl.ds(0, 2)], load_sem.at[2])

    top = jnp.max(meta[:, 0, : 3 * COLS], axis=0, keepdims=True)
    for m, factor in enumerate((factor_q, factor_k, factor_v)):
        of_m = top[:, m * COLS : (m + 1) * COLS]
        factor[...] = of_m[0]
        inverse[m] = 1.0 / of_m

    def scale_own(m, r, size):
        scaled = fresh[m, pl.ds(r, size)] * inverse[m]
        at = pl.multiple_of(row_of(m, r, z), 32)
        out[pl.ds(at, size)] = scaled.astype(jnp.bfloat16)

    for j in range(NPIECE):
        scale_own(*PIECES[j])
        if j > 0:
            send((SCALED, j - 1, 1))
    scale_own(0, 0, ROWS)
    send((SCALED, NPIECE - 1, 1))

    def hop(n, buf, at, axis, recv):
        slot, step = ((at, 1), (at, -1), (lax.rem(at + 3, 4), 1))[n]
        return pltpu.make_async_remote_copy(
            src_ref=buf.at[slot], dst_ref=buf.at[slot], send_sem=sends.at[0],
            recv_sem=recv.at[0 if n == 0 else 1], device_id=beside(axis, at, step, 4), device_id_type=MESH,
        )

    low_x = (lowx, x, "width_1", x_r)
    gain_x = (norm_x, x, "width_1", x_r)
    gain_y = (norm_y, y, "width_0", y_r)

    def begin(*ring):
        hop(0, *ring).start()
        hop(1, *ring).start()

    def sizes(n, *rings):
        return out.at[pl.ds(0, n * sum(8 if ring[0] is not lowx else 64 for ring in rings))]

    def pass_on(*rings):
        all_of(sizes(1, *rings), rings[0][-1].at[0])
        for ring in rings:
            hop(2, *ring).start()

    def complete(*rings):
        all_of(sizes(2, *rings), rings[0][-1].at[1])

    all_of(lowx.at[0, pl.ds(0, 2)], low_last)
    norm_x[x] = meta[:, 0, 3 * COLS : 3 * COLS + 128]
    for n, (_, at) in enumerate(plane):
        @pl.when(at < 3)
        def _(n=n):
            pl.semaphore_wait(ready.at[n], 2 - lower[n])
    begin(*low_x)
    begin(*gain_x)

    def scale_raw(back):
        o = lax.rem(z + back, Z)
        for b in range(NBLOCK):
            rows = pl.ds(b * BLOCK, BLOCK)
            block = fresh_of(lowx[b, o], high[0], rawx[o, rows])
            at = pl.multiple_of(row_of(0, b * BLOCK, o), BLOCK)
            out[pl.ds(at, BLOCK)] = (block * inverse[0]).astype(jnp.bfloat16)

    send(*raw(4, 1, 2, 3))
    pass_on(low_x, gain_x)
    send((SCALED, 0, 2), (SCALED, 1, 2))
    complete(low_x, gain_x)
    norm_y[y] = jnp.sum(norm_x[...], axis=0)
    begin(*gain_y)
    scale_raw(1)
    scale_raw(7)
    pass_on(gain_y)
    scale_raw(2)
    scale_raw(6)
    send((SCALED, 2, 2))
    scale_raw(3)
    scale_raw(5)
    complete(gain_y)
    for s in range(4):
        for t in range(Z):
            norm_all[pl.ds(t * 4 + s, 1)] = norm_y[s, pl.ds(t, 1)]
    norm[...] = norm_all[...].astype(jnp.bfloat16)
    send((SCALED, 0, 3))
    all_of(rawx.at[0], load_sem.at[1])
    scale_raw(4)
    send(*[(SCALED, n, 3) for n in range(1, NPIECE)])

    send((SCALED, 0, 4))
    end = 1
    for d in (0, 1):
        arrived_one(SCALED, end, 3, d)
    piece_copy(1, 4, end).start()
    usual, moved = piece_copy(0, 4, end, MOVED), piece_copy(1, 4, end, MOVED, 0)

    @pl.when(z < Z - 1)
    def _():
        usual.start()

    @pl.when(z == 1)
    def _():
        moved.start()

    send((SCALED, 2, 4))
    all_of(out.at[pl.ds(0, 2 * ROWS)], load_sem.at[0])

    all_of(out.at[pl.ds(0, 21 * ROWS - PIECE // 2 + 14 * 8 + 3 * (64 + 8 + 8))], sends.at[0])

    @pl.when(jnp.logical_and(z != 1, z < Z - 1))
    def _():
        usual.wait_send()

    @pl.when(z == 1)
    def _():
        all_of(out.at[pl.ds(0, PIECE)], sends.at[1])


def write_kernel(weights, fq, fk, fv, gain, sq, sk, sv, oq, ok, ov, og, sem):
    writes = [
        pltpu.make_async_copy(src, dst, sem.at[n])
        for n, (src, dst) in enumerate((
            (weights.at[pl.ds(0, WHOLE)], sq), (weights.at[pl.ds(WHOLE, WHOLE)], sk),
            (weights.at[pl.ds(2 * WHOLE, WHOLE)], sv), (fq, oq), (fk, ok), (fv, ov), (gain, og),
        ))
    ]
    for write in writes:
        write.start()
    for write in writes:
        write.wait()


def per_device(tq, lq, hq, tk, lk, hk, tv, lv, hv, nt, ns):
    hbm = pl.BlockSpec(memory_space=pltpu.HBM)
    vmem = pl.BlockSpec(memory_space=pltpu.VMEM)
    dma = pltpu.SemaphoreType.DMA
    f32, bf16 = jnp.float32, jnp.bfloat16
    args = (tq, lq.T, hq, tk, lk.T, hk, tv, lv.T, hv, nt.reshape(1, 32), ns.reshape(1, 32))
    gathered = pl.pallas_call(
        gather_kernel,
        name="gather_z",
        out_shape=(pltpu.VMEM((3 * WHOLE, COLS), bf16),)
        + (pltpu.VMEM((COLS,), f32),) * 3
        + (pltpu.VMEM((32, 128), bf16),),
        in_specs=[hbm] * 11,
        out_specs=(vmem,) * 5,
        scratch_shapes=[
            pltpu.VMEM((3, ROWS, COLS), bf16),
            pltpu.VMEM((3, 16, ROWS), bf16),
            pltpu.VMEM((3, 16, COLS), bf16),
            pltpu.VMEM((2, 1, 32), f32),
            pltpu.VMEM((3, ROWS, COLS), f32),
            pltpu.VMEM((Z, ROWS, COLS), bf16),
            pltpu.VMEM((4, Z, 16, BLOCK), bf16),
            pltpu.VMEM((Z, 1, META), f32),
            pltpu.VMEM((4, Z, 128), f32),
            pltpu.VMEM((4, Z, 128), f32),
            pltpu.VMEM((32, 128), f32),
            pltpu.VMEM((3, 1, COLS), f32),
            dma((3,)), dma((2,)),
            dma((2, 3, NBLOCK)), dma((5,)), dma((5,)), dma,
            dma((2,)), dma((2,)),
            pltpu.SemaphoreType.REGULAR((3,)),
        ],
        compiler_params=pltpu.CompilerParams(
            collective_id=0, has_side_effects=True, vmem_limit_bytes=32 * 1024 * 1024
        ),
    )(*[pltpu.with_memory_space_constraint(a, pltpu.HBM) for a in args])
    shapes = ((WHOLE, COLS), bf16), ((COLS,), f32)
    sq, sk, sv, fq, fk, fv, gain = pl.pallas_call(
        write_kernel,
        name="write_out",
        out_shape=(jax.ShapeDtypeStruct(*shapes[0]),) * 3
        + (jax.ShapeDtypeStruct(*shapes[1]),) * 3
        + (jax.ShapeDtypeStruct((32, 128), bf16),),
        in_specs=[vmem] * 5,
        out_specs=(hbm,) * 7,
        scratch_shapes=[dma((7,))],
        compiler_params=pltpu.CompilerParams(vmem_limit_bytes=16 * 1024 * 1024),
    )(*gathered)
    return sq, sk, sv, fq, fk, fv, gain.reshape(4096)


def solution(mesh):
    finer = Mesh(
        mesh.devices.reshape(mesh.shape["zero"], 4, 4, mesh.shape["unit"]),
        ("zero", "width_0", "width_1", "unit"),
    )
    matrix, low, high = P(("unit", "zero"), WIDTH), P(("unit", "zero"), None), P("unit", WIDTH)
    return jax.shard_map(
        per_device,
        mesh=finer,
        in_specs=(matrix, low, high) * 3 + (P(UNIT_ZERO_WIDTH), P(UNIT_ZERO_WIDTH)),
        out_specs=(high, high, high, P(UNIT_WIDTH), P(UNIT_WIDTH), P(UNIT_WIDTH), P("unit")),
        check_vma=False,
    )
```

```python
import functools

import jax
import jax.numpy as jnp
from jax import lax
from jax.experimental import pallas as pl
from jax.experimental.pallas import tpu as pltpu
from jax.sharding import Mesh
from jax.sharding import PartitionSpec as P

WIDTH = ("width_0", "width_1")
UNIT_ZERO_WIDTH = ("unit", "zero", "width_0", "width_1")
UNIT_WIDTH = ("unit", "width_0", "width_1")
MESH = pl.DeviceIdType.MESH

mix_rate = 1.0

Z = 8
ROWS = 512
COLS = 256
WHOLE = Z * ROWS
BLOCK = 128
NBLOCK = ROWS // BLOCK
PIECES = ((1, 0, 512), (2, 0, 320), (2, 320, 192))
NPIECE = len(PIECES)
PIECE = 320
META = 3 * COLS + 128
RAW, SCALED, LOW, TOP, MOVED = range(5)


def fresh_of(low_t, high, train):
    product = lax.dot_general(
        low_t, high, (((0,), (0,)), ((), ())), preferred_element_type=jnp.float32
    )
    return train.astype(jnp.float32) + mix_rate * product


def gather_kernel(
    tq, lq, hq, tk, lk, hk, tv, lv, hv, nt, ns,
    out, factor_q, factor_k, factor_v, norm,
    train, low, high, norm_in, fresh, rawx, lowx, meta, norm_x, norm_y, norm_all, inverse,
    load_sem, sends, arrivals, meta_r, low_r, low_last, x_r, y_r, ready,
):
    z = lax.axis_index("zero")
    y = lax.axis_index("width_0")
    x = lax.axis_index("width_1")

    lanes = pl.ds(pl.multiple_of(x * BLOCK, BLOCK), BLOCK)
    groups = (
        ((tq, train.at[0]),),
        (
            (tk, train.at[1]), (tv, train.at[2]), (lq, low.at[0]), (lk, low.at[1]), (lv, low.at[2]),
            (hq, high.at[0]), (hk, high.at[1]), (hv, high.at[2]), (lq.at[:, lanes], lowx.at[x, z]),
        ),
        ((nt, norm_in.at[0]), (ns, norm_in.at[1])),
    )
    for n, group in enumerate(groups):
        for src, dst in group:
            pltpu.make_async_copy(src, dst, load_sem.at[n]).start()

    def all_of(ref, sem):
        pltpu.make_async_copy(ref, ref, sem).wait()

    def beside(axis, at, step, size):
        return {axis: lax.rem(at + (step + size), size)}

    towards = (beside("zero", z, 1, Z), beside("zero", z, -1, Z))
    barrier = pltpu.get_barrier_semaphore()
    pl.semaphore_signal(barrier, inc=1, device_id=towards[1], device_id_type=MESH)

    @pl.when(z < Z - 1)
    def _():
        pl.semaphore_signal(barrier, inc=1, device_id=towards[0], device_id_type=MESH)

    plane = (("width_1", x), ("width_0", y))
    for axis, at in plane:
        @pl.when(at < 3)
        def _(axis=axis, at=at):
            pl.semaphore_signal(barrier, inc=1, device_id={axis: lax.rem(at + 1, 4)}, device_id_type=MESH)

        @pl.when(at == 0)
        def _(axis=axis, at=at):
            pl.semaphore_signal(barrier, inc=1, device_id={axis: lax.rem(at + 3, 4)}, device_id_type=MESH)

    lower = [(at + 1) // 2 for _, at in plane]
    pl.semaphore_wait(barrier, 1 + lax.min(z, 1) + lower[0] + lower[1])

    @pl.when(z == Z - 1)
    def _():
        pl.semaphore_signal(ready.at[2], inc=1, device_id=towards[0], device_id_type=MESH)

    def answer():
        for n, (axis, at) in enumerate(plane):
            @pl.when(at > 0)
            def _(n=n, axis=axis, at=at):
                pl.semaphore_signal(ready.at[n], inc=1, device_id={axis: lax.rem(at + 3, 4)}, device_id_type=MESH)

            @pl.when(at == 3)
            def _(n=n, axis=axis, at=at):
                pl.semaphore_signal(ready.at[n], inc=1, device_id={axis: lax.rem(at + 1, 4)}, device_id_type=MESH)

    def origin(d, h):
        back = h - 1
        return lax.rem(z + (Z - back if d == 0 else back), Z)

    def remote(src, dst, kind, recv, d):
        return pltpu.make_async_remote_copy(
            src_ref=src, dst_ref=dst, send_sem=sends.at[2 if kind == TOP else kind // MOVED], recv_sem=recv,
            device_id=towards[d], device_id_type=MESH,
        )

    def half(start, size, d, h):
        return (start, size) if h < 4 else (start + d * (size // 2), size // 2)

    def raw_copy(d, h, n):
        at, size = half(n * BLOCK, BLOCK, d, h)
        there = rawx.at[origin(d, h), pl.ds(at, size)]
        here = train.at[0, pl.ds(at, size)] if h == 1 else there
        recv = arrivals.at[d, h - 1, n] if h < 4 else load_sem.at[1]
        return remote(here, there, RAW, recv, d)

    def low_copy(d, h, n):
        ref = lowx.at[x, origin(d, h)]
        recv = low_last if ends(LOW, d, h) else low_r.at[2 * h - 1 - d]
        return remote(ref, ref, LOW, recv, d)

    def meta_copy(d, h, n):
        ref = meta.at[origin(d, h)]
        recv = load_sem.at[2] if ends(TOP, d, h) else meta_r.at[2 * h - 2 + d]
        return remote(ref, ref, TOP, recv, d)

    def row_of(m, r, o):
        return m * WHOLE + o * ROWS + r

    def piece_copy(d, h, n, kind=SCALED, part=None):
        m, r, size = PIECES[n]
        at, size = half(row_of(m, r, origin(d, h)), size, d if part is None else part, h)
        ref = out.at[pl.ds(pl.multiple_of(at, 32), size)]
        recv = arrivals.at[d, h - 1, n] if h < 4 else load_sem.at[0]
        return remote(ref, ref, kind, recv, d)

    copy_of = (raw_copy, piece_copy, low_copy, meta_copy)

    def goes(kind, h, d):
        return h < 4 or kind in (RAW, SCALED) or d == (1 if kind == LOW else 0)

    def ends(kind, d, h):
        return not goes(kind, h + 1, d) if h < 4 else True

    landed = set()

    def arrived_one(kind, n, h, d):
        if (kind, n, h, d) not in landed and not ends(kind, d, h):
            landed.add((kind, n, h, d))
            copy_of[kind](d, h, n).wait_recv()

    def send(*items):
        for kind, n, h in items:
            for d in (0, 1):
                if h > 1:
                    arrived_one(kind, n, h - 1, d)
                if goes(kind, h, d):
                    copy_of[kind](d, h, n).start()

    def raw(h, *pieces):
        return [(RAW, n, h) for n in pieces]

    def small(h):
        return [(LOW, 0, h), (TOP, 0, h)]

    all_of(train.at[0], load_sem.at[0])
    raw_copy(0, 1, 0).start()
    raw_copy(0, 1, 1).start()

    @pl.when(z == 0)
    def _():
        pl.semaphore_wait(ready.at[2], 1)

    raw_copy(1, 1, 0).start()
    raw_copy(1, 1, 1).start()
    answer()
    all_of(out.at[pl.ds(0, 2 * ROWS + 152)], load_sem.at[1])
    all_of(norm_in, load_sem.at[2])
    for m in range(3):
        top = jnp.zeros((8, COLS), jnp.float32)
        for b in range(ROWS // BLOCK):
            rows = pl.ds(b * BLOCK, BLOCK)
            block = fresh_of(low[m, :, rows], high[m], train[m, rows])
            fresh[m, rows] = block
            top = jnp.maximum(top, jnp.max(jnp.abs(block).reshape(BLOCK // 8, 8, COLS), axis=0))
        meta[z, :, pl.ds(m * COLS, COLS)] = jnp.max(top, axis=0, keepdims=True)
    gain = (norm_in[0] + norm_in[1]).astype(jnp.bfloat16)
    lane = lax.broadcasted_iota(jnp.int32, (32, 128), 1)
    entry = lax.broadcasted_iota(jnp.int32, (32, 128), 0)
    place = (lane == entry + 32 * x).astype(jnp.bfloat16)
    meta[z, :, pl.ds(3 * COLS, 128)] = jnp.dot(gain, place, preferred_element_type=jnp.float32)

    send(*small(1), *raw(1, 2, 3), *raw(2, 0))
    send(*small(2), *raw(2, 1, 2))
    send(*small(3), *raw(2, 3), *raw(3, 0, 1))
    send(*small(4), *raw(3, 2, 3), *raw(4, 0))
    all_of(meta.at[pl.ds(0, 2)], load_sem.at[2])

    top = jnp.max(meta[:, 0, : 3 * COLS], axis=0, keepdims=True)
    for m, factor in enumerate((factor_q, factor_k, factor_v)):
        of_m = top[:, m * COLS : (m + 1) * COLS]
        factor[...] = of_m[0]
        inverse[m] = 1.0 / of_m

    def scale_own(m, r, size):
        scaled = fresh[m, pl.ds(r, size)] * inverse[m]
        at = pl.multiple_of(row_of(m, r, z), 32)
        out[pl.ds(at, size)] = scaled.astype(jnp.bfloat16)

    for j in range(NPIECE):
        scale_own(*PIECES[j])
        if j > 0:
            send((SCALED, j - 1, 1))
    scale_own(0, 0, ROWS)
    send((SCALED, NPIECE - 1, 1))

    def hop(n, buf, at, axis, recv):
        slot, step = ((at, 1), (at, -1), (lax.rem(at + 3, 4), 1))[n]
        return pltpu.make_async_remote_copy(
            src_ref=buf.at[slot], dst_ref=buf.at[slot], send_sem=sends.at[0],
            recv_sem=recv.at[0 if n == 0 else 1], device_id=beside(axis, at, step, 4), device_id_type=MESH,
        )

    low_x = (lowx, x, "width_1", x_r)
    gain_x = (norm_x, x, "width_1", x_r)
    gain_y = (norm_y, y, "width_0", y_r)

    def begin(*ring):
        hop(0, *ring).start()
        hop(1, *ring).start()

    def sizes(n, *rings):
        return out.at[pl.ds(0, n * sum(8 if ring[0] is not lowx else 64 for ring in rings))]

    def pass_on(*rings):
        all_of(sizes(1, *rings), rings[0][-1].at[0])
        for ring in rings:
            hop(2, *ring).start()

    def complete(*rings):
        all_of(sizes(2, *rings), rings[0][-1].at[1])

    all_of(lowx.at[0, pl.ds(0, 2)], low_last)
    norm_x[x] = meta[:, 0, 3 * COLS : 3 * COLS + 128]
    for n, (_, at) in enumerate(plane):
        @pl.when(at < 3)
        def _(n=n):
            pl.semaphore_wait(ready.at[n], 2 - lower[n])
    begin(*low_x)
    begin(*gain_x)

    def scale_raw(back):
        o = lax.rem(z + back, Z)
        for b in range(NBLOCK):
            rows = pl.ds(b * BLOCK, BLOCK)
            block = fresh_of(lowx[b, o], high[0], rawx[o, rows])
            at = pl.multiple_of(row_of(0, b * BLOCK, o), BLOCK)
            out[pl.ds(at, BLOCK)] = (block * inverse[0]).astype(jnp.bfloat16)

    send(*raw(4, 1, 2, 3))
    pass_on(low_x, gain_x)
    send((SCALED, 0, 2), (SCALED, 1, 2))
    complete(low_x, gain_x)
    norm_y[y] = jnp.sum(norm_x[...], axis=0)
    begin(*gain_y)
    scale_raw(1)
    scale_raw(7)
    pass_on(gain_y)
    scale_raw(2)
    scale_raw(6)
    send((SCALED, 2, 2))
    scale_raw(3)
    scale_raw(5)
    complete(gain_y)
    for s in range(4):
        for t in range(Z):
            norm_all[pl.ds(t * 4 + s, 1)] = norm_y[s, pl.ds(t, 1)]
    norm[...] = norm_all[...].astype(jnp.bfloat16)
    send((SCALED, 0, 3))
    all_of(rawx.at[0], load_sem.at[1])
    scale_raw(4)
    send(*[(SCALED, n, 3) for n in range(1, NPIECE)])

    send((SCALED, 0, 4))
    end = 1
    for d in (0, 1):
        arrived_one(SCALED, end, 3, d)
    piece_copy(1, 4, end).start()
    usual, moved = piece_copy(0, 4, end, MOVED), piece_copy(1, 4, end, MOVED, 0)

    @pl.when(z < Z - 1)
    def _():
        usual.start()

    @pl.when(z == 1)
    def _():
        moved.start()

    send((SCALED, 2, 4))
    all_of(out.at[pl.ds(0, 2 * ROWS)], load_sem.at[0])

    all_of(out.at[pl.ds(0, 21 * ROWS - PIECE // 2 + 7 * 8 + 3 * (64 + 8 + 8))], sends.at[0])
    all_of(meta.at[pl.ds(0, 7)], sends.at[2])

    @pl.when(jnp.logical_and(z != 1, z < Z - 1))
    def _():
        usual.wait_send()

    @pl.when(z == 1)
    def _():
        all_of(out.at[pl.ds(0, PIECE)], sends.at[1])


def write_kernel(weights, fq, fk, fv, gain, sq, sk, sv, oq, ok, ov, og, sem):
    for m, dst in enumerate((sq, sk, sv)):
        pltpu.make_async_copy(weights.at[pl.ds(m * WHOLE, WHOLE)], dst, sem.at[0]).start()
    rest = [
        pltpu.make_async_copy(src, dst, sem.at[1 + n])
        for n, (src, dst) in enumerate(((fq, oq), (fk, ok), (fv, ov), (gain, og)))
    ]
    for write in rest:
        write.start()
    for write in rest:
        write.wait()
    pltpu.make_async_copy(weights, weights, sem.at[0]).wait()


def per_device(tq, lq, hq, tk, lk, hk, tv, lv, hv, nt, ns):
    hbm = pl.BlockSpec(memory_space=pltpu.HBM)
    vmem = pl.BlockSpec(memory_space=pltpu.VMEM)
    dma = pltpu.SemaphoreType.DMA
    f32, bf16 = jnp.float32, jnp.bfloat16
    args = (tq, lq.T, hq, tk, lk.T, hk, tv, lv.T, hv, nt.reshape(1, 32), ns.reshape(1, 32))
    gathered = pl.pallas_call(
        gather_kernel,
        name="gather_z",
        out_shape=(pltpu.VMEM((3 * WHOLE, COLS), bf16),)
        + (pltpu.VMEM((COLS,), f32),) * 3
        + (pltpu.VMEM((32, 128), bf16),),
        in_specs=[hbm] * 11,
        out_specs=(vmem,) * 5,
        scratch_shapes=[
            pltpu.VMEM((3, ROWS, COLS), bf16),
            pltpu.VMEM((3, 16, ROWS), bf16),
            pltpu.VMEM((3, 16, COLS), bf16),
            pltpu.VMEM((2, 1, 32), f32),
            pltpu.VMEM((3, ROWS, COLS), f32),
            pltpu.VMEM((Z, ROWS, COLS), bf16),
            pltpu.VMEM((4, Z, 16, BLOCK), bf16),
            pltpu.VMEM((Z, 1, META), f32),
            pltpu.VMEM((4, Z, 128), f32),
            pltpu.VMEM((4, Z, 128), f32),
            pltpu.VMEM((32, 128), f32),
            pltpu.VMEM((3, 1, COLS), f32),
            dma((3,)), dma((3,)),
            dma((2, 3, NBLOCK)), dma((5,)), dma((5,)), dma,
            dma((2,)), dma((2,)),
            pltpu.SemaphoreType.REGULAR((3,)),
        ],
        compiler_params=pltpu.CompilerParams(
            collective_id=0, has_side_effects=True, vmem_limit_bytes=32 * 1024 * 1024
        ),
    )(*[pltpu.with_memory_space_constraint(a, pltpu.HBM) for a in args])
    shapes = ((WHOLE, COLS), bf16), ((COLS,), f32)
    sq, sk, sv, fq, fk, fv, gain = pl.pallas_call(
        write_kernel,
        name="write_out",
        out_shape=(jax.ShapeDtypeStruct(*shapes[0]),) * 3
        + (jax.ShapeDtypeStruct(*shapes[1]),) * 3
        + (jax.ShapeDtypeStruct((32, 128), bf16),),
        in_specs=[vmem] * 5,
        out_specs=(hbm,) * 7,
        scratch_shapes=[dma((5,))],
        compiler_params=pltpu.CompilerParams(vmem_limit_bytes=16 * 1024 * 1024),
    )(*gathered)
    return sq, sk, sv, fq, fk, fv, gain.reshape(4096)


def solution(mesh):
    finer = Mesh(
        mesh.devices.reshape(mesh.shape["zero"], 4, 4, mesh.shape["unit"]),
        ("zero", "width_0", "width_1", "unit"),
    )
    matrix, low, high = P(("unit", "zero"), WIDTH), P(("unit", "zero"), None), P("unit", WIDTH)
    return jax.shard_map(
        per_device,
        mesh=finer,
        in_specs=(matrix, low, high) * 3 + (P(UNIT_ZERO_WIDTH), P(UNIT_ZERO_WIDTH)),
        out_specs=(high, high, high, P(UNIT_WIDTH), P(UNIT_WIDTH), P(UNIT_WIDTH), P("unit")),
        check_vma=False,
    )
```
